16 devices in a mesh: dp: 2 (over y, z), tp: 8 (over x, core).
Axes of the slice: x: 4, y: 2, z: 1, core: 2. Of those that a mesh axis runs over, the one named last changes fastest.
The devices are a block of a 4x4x8 slice.
Arguments:
- tok_hidden: bfloat16 [256, 2048], P('dp'), parts along dimension 0
- seq_lens: int32 [256], P('dp'), parts along dimension 0
- k_cache: bfloat16 [256, 512, 8, 64], P('dp', None, 'tp'), parts along dimension 0
- v_cache: bfloat16 [256, 512, 8, 64], P('dp', None, 'tp'), parts along dimension 0
- next_tok: int32 [256], P('dp'), parts along dimension 0
- g_attn: bfloat16 [2048], replicated
- w_q: bfloat16 [2048, 2048], P(None, 'tp')
- b_q: bfloat16 [2048], P('tp')
- w_k: bfloat16 [2048, 512], P(None, 'tp')
- b_k: bfloat16 [512], P('tp')
- w_v: bfloat16 [2048, 512], P(None, 'tp')
- b_v: bfloat16 [512], P('tp')
- w_o: bfloat16 [2048, 2048], P('tp')
- g_mlp: bfloat16 [2048], replicated
- w_gate: bfloat16 [2048, 8192], P(None, 'tp')
- w_up: bfloat16 [2048, 8192], P(None, 'tp')
- w_down: bfloat16 [8192, 2048], P('tp')
- g_final: bfloat16 [2048], replicated
- w_head: bfloat16 [128256, 2048], P('tp')
Outputs:
- output 1: bfloat16 [256, 2048], P('dp'), parts along dimension 0
- output 2: bfloat16 [256, 512, 8, 64], P('dp', None, 'tp'), parts along dimension 0
- output 3: bfloat16 [256, 512, 8, 64], P('dp', None, 'tp'), parts along dimension 0
- output 4: float32 [256], P('dp'), parts along dimension 0
- output 5: float32 [256], P('dp'), parts along dimension 0
There are 2 independent parts. The reference program is written for one: setup_inputs(seed, part) draws one part's arguments, and reference() takes and returns one part's arrays. A program takes and returns all parts, laid end to end along the dimension named above; an argument that names none is the same for every part.
All inputs are finite; a program needn't handle non-finite values.
Results may differ from the reference program's by a relative error of at most 0.0139837.
Values are sent between devices in bfloat16 or wider.
A program may use at most 768 MiB of HBM per device.

```python
import math
import jax
import jax.numpy as jnp
from jax import lax

BATCH = 128
LMAX = 512
D = 2048
HEADS = 32
KV_HEADS = 8
HEAD = 64
FF = 8192
VOCAB = 128256
KV_SLOTS = 8
THETA = 1000000
EPS = 1e-6
COPIES = KV_SLOTS // KV_HEADS
GROUP = HEADS // KV_SLOTS


def rms_norm(values, gain_vec):
    vals_f32 = values.astype(jnp.float32)
    inv_rms = lax.rsqrt(jnp.mean(vals_f32 * vals_f32, axis=-1, keepdims=True) + EPS)
    return (vals_f32 * inv_rms * gain_vec.astype(jnp.float32)).astype(jnp.bfloat16)


def rotary(values, positions):
    half_dim = values.shape[-1] // 2
    inv_freq = jnp.power(float(THETA), jnp.arange(half_dim, dtype=jnp.float32) * (-2.0 / values.shape[-1]))
    angles = positions.astype(jnp.float32)[:, None] * inv_freq[None, :]
    cos_part = jnp.cos(angles)[:, None, :]
    sin_part = jnp.sin(angles)[:, None, :]
    first_half = values[..., :half_dim]
    second_half = values[..., half_dim:]
    return jnp.concatenate([first_half * cos_part - second_half * sin_part, second_half * cos_part + first_half * sin_part], axis=-1)


def draw_lengths(len_key):
    exp_key, off_key, pick_key = jax.random.split(len_key, 3)
    log_max = int(math.log2(LMAX))
    exponent = jax.random.randint(exp_key, (BATCH,), 0, log_max)
    base_len = jnp.left_shift(jnp.ones((BATCH,), jnp.int32), exponent)
    offset = jax.random.randint(off_key, (BATCH,), 0, LMAX) % base_len
    longest = jax.random.randint(pick_key, (), 0, BATCH)
    return jnp.where(jnp.arange(BATCH) == longest, LMAX - 1, base_len + offset).astype(jnp.int32)


def gaussian(rand_key, arr_shape, spread):
    return jax.random.normal(rand_key, arr_shape, jnp.float32) * spread


def setup_inputs(seed: int = 0, part: int = 0) -> dict:
    shared_keys = jax.random.split(jax.random.key(seed), 16)
    part_keys = jax.random.split(jax.random.fold_in(jax.random.key(seed + 1), part), 8)
    k_scale = math.sqrt(max(math.log(LMAX / 8.0), 1.0) / 1.25)
    k_base = gaussian(part_keys[2], (BATCH, LMAX, KV_HEADS, HEAD), k_scale)
    v_base = gaussian(part_keys[3], (BATCH, LMAX, KV_HEADS, HEAD), 1.0)
    w_k = gaussian(shared_keys[3], (D, KV_HEADS, HEAD), D ** -0.5)
    b_k = gaussian(shared_keys[4], (KV_HEADS, HEAD), 0.5)
    w_v = gaussian(shared_keys[5], (D, KV_HEADS, HEAD), D ** -0.5)
    b_v = gaussian(shared_keys[6], (KV_HEADS, HEAD), 0.5)
    return {
        'tok_hidden': gaussian(part_keys[0], (BATCH, D), 1.0).astype(jnp.bfloat16),
        'seq_lens': draw_lengths(part_keys[1]),
        'k_cache': jnp.repeat(k_base, COPIES, axis=2).astype(jnp.bfloat16),
        'v_cache': jnp.repeat(v_base, COPIES, axis=2).astype(jnp.bfloat16),
        'next_tok': jax.random.randint(part_keys[4], (BATCH,), 0, VOCAB),
        'g_attn': (1.0 + gaussian(shared_keys[0], (D,), 0.2)).astype(jnp.bfloat16),
        'w_q': gaussian(shared_keys[1], (D, HEADS * HEAD), D ** -0.5).astype(jnp.bfloat16),
        'b_q': gaussian(shared_keys[2], (HEADS * HEAD,), 0.5).astype(jnp.bfloat16),
        'w_k': jnp.repeat(w_k, COPIES, axis=1).reshape(D, KV_SLOTS * HEAD).astype(jnp.bfloat16),
        'b_k': jnp.repeat(b_k, COPIES, axis=0).reshape(KV_SLOTS * HEAD).astype(jnp.bfloat16),
        'w_v': jnp.repeat(w_v, COPIES, axis=1).reshape(D, KV_SLOTS * HEAD).astype(jnp.bfloat16),
        'b_v': jnp.repeat(b_v, COPIES, axis=0).reshape(KV_SLOTS * HEAD).astype(jnp.bfloat16),
        'w_o': gaussian(shared_keys[7], (HEADS * HEAD, D), (HEADS * HEAD) ** -0.5).astype(jnp.bfloat16),
        'g_mlp': (1.0 + gaussian(shared_keys[8], (D,), 0.2)).astype(jnp.bfloat16),
        'w_gate': gaussian(shared_keys[9], (D, FF), D ** -0.5).astype(jnp.bfloat16),
        'w_up': gaussian(shared_keys[10], (D, FF), D ** -0.5).astype(jnp.bfloat16),
        'w_down': gaussian(shared_keys[11], (FF, D), FF ** -0.5).astype(jnp.bfloat16),
        'g_final': (3.0 + gaussian(shared_keys[12], (D,), 0.5)).astype(jnp.bfloat16),
        'w_head': gaussian(shared_keys[13], (VOCAB, D), D ** -0.5).astype(jnp.bfloat16),
    }


def reference(tok_hidden, seq_lens, k_cache, v_cache, next_tok, g_attn, w_q, b_q, w_k, b_k, w_v, b_v, w_o, g_mlp, w_gate, w_up, w_down, g_final, w_head):
    normed = rms_norm(tok_hidden, g_attn)
    q_proj = jnp.dot(normed, w_q, preferred_element_type=jnp.float32) + b_q.astype(jnp.float32)
    k_proj = jnp.dot(normed, w_k, preferred_element_type=jnp.float32) + b_k.astype(jnp.float32)
    v_proj = jnp.dot(normed, w_v, preferred_element_type=jnp.float32) + b_v.astype(jnp.float32)
    q_rot = rotary(q_proj.reshape(BATCH, HEADS, HEAD), seq_lens).astype(jnp.bfloat16)
    k_new = rotary(k_proj.reshape(BATCH, KV_SLOTS, HEAD), seq_lens).astype(jnp.bfloat16)
    v_new = v_proj.reshape(BATCH, KV_SLOTS, HEAD).astype(jnp.bfloat16)
    slot_ids = jnp.arange(LMAX)
    write_mask = (slot_ids[None, :] == seq_lens[:, None])[:, :, None, None]
    k_all = jnp.where(write_mask, k_new[:, None], k_cache)
    v_all = jnp.where(write_mask, v_new[:, None], v_cache)

    def one_row(row_args):
        q_row, k_row, v_row, length = row_args
        q_grp = q_row.reshape(KV_SLOTS, GROUP, HEAD).astype(jnp.float32)
        scores = jnp.einsum('kgd,lkd->kgl', q_grp, k_row.astype(jnp.float32)) * (HEAD ** -0.5)
        scores = jnp.where((slot_ids <= length)[None, None, :], scores, -jnp.inf)
        attn_probs = jax.nn.softmax(scores, axis=-1).astype(jnp.bfloat16).astype(jnp.float32)
        attn_vals = jnp.einsum('kgl,lkd->kgd', attn_probs, v_row.astype(jnp.float32))
        return attn_vals.reshape(HEADS * HEAD).astype(jnp.bfloat16)

    attn_out = lax.map(one_row, (q_rot, k_all, v_all, seq_lens))
    attn_proj = jnp.dot(attn_out, w_o, preferred_element_type=jnp.float32)
    residual = (tok_hidden.astype(jnp.float32) + attn_proj).astype(jnp.bfloat16)
    mlp_in = rms_norm(residual, g_mlp)
    gate_proj = jnp.dot(mlp_in, w_gate, preferred_element_type=jnp.float32)
    up_proj = jnp.dot(mlp_in, w_up, preferred_element_type=jnp.float32)
    hidden = (jax.nn.silu(gate_proj) * up_proj).astype(jnp.bfloat16)
    down_proj = jnp.dot(hidden, w_down, preferred_element_type=jnp.float32)
    y_out = (residual.astype(jnp.float32) + down_proj).astype(jnp.bfloat16)
    final_norm = rms_norm(y_out, g_final)
    logits = lax.dot_general(final_norm, w_head, (((1,), (1,)), ((), ())), preferred_element_type=jnp.float32)
    norm_lse = jax.nn.logsumexp(logits, axis=-1)
    vocab_ids = jnp.arange(VOCAB)
    target = jnp.sum(jnp.where(vocab_ids[None, :] == next_tok[:, None], logits, 0.0), axis=-1)
    tok_logp = target - norm_lse
    return (y_out, k_all, v_all, tok_logp, norm_lse)
```

```python
import functools
import numpy as np
import jax
import jax.numpy as jnp
from jax import lax
from jax.experimental import pallas as pl
from jax.experimental.pallas import tpu as pltpu
from jax.sharding import PartitionSpec as P

THETA = 1000000.0
EPS = 1e-6
MESH = pl.DeviceIdType.MESH
NT = (((1,), (1,)), ((), ()))
F32 = jnp.float32
BF16 = jnp.bfloat16


def rms(vals_f32, gain_f32):
    inv_rms = lax.rsqrt(jnp.mean(vals_f32 * vals_f32, axis=-1, keepdims=True) + EPS)
    return (vals_f32 * inv_rms * gain_f32).astype(BF16)


SEQ = 8
SUB = 2


def attn_kernel(lens_s, lens_v, x_ref, g_ref, bq_ref, bk_ref, bv_ref, freq_ref, kc, vc, wq, wk, wv, wo,
                ko, vo, part, kbuf, vbuf, wq_v, wkv_v, wo_v, lens_b, qq, kvt, o_s,
                k_in, v_in, k_out, v_out, w_sem):
    rows = x_ref.shape[0]
    dim = wk.shape[0]
    slots = kbuf.shape[1]
    span = SEQ * SUB * dim
    steps = kbuf.shape[0] // span

    w_copies = [pltpu.make_async_copy(wq, wq_v, w_sem.at[0]),
                pltpu.make_async_copy(wk, wkv_v.at[pl.ds(0, dim)], w_sem.at[1]),
                pltpu.make_async_copy(wv, wkv_v.at[pl.ds(dim, dim)], w_sem.at[2])]
    wo_copy = pltpu.make_async_copy(wo, wo_v, w_sem.at[3])
    for copy in w_copies:
        copy.start()

    def moves(step):
        here = pl.ds(pl.multiple_of(step * span, span), span)
        return (pltpu.make_async_copy(kc.at[here], kbuf.at[here], k_in.at[step]),
                pltpu.make_async_copy(vc.at[here], vbuf.at[here], v_in.at[step]),
                pltpu.make_async_copy(kbuf.at[here], ko.at[here], k_out.at[step]),
                pltpu.make_async_copy(vbuf.at[here], vo.at[here], v_out.at[step]))

    def begin(step, carry):
        k_copy, v_copy, _, _ = moves(step)
        k_copy.start()
        v_copy.start()
        return carry

    lax.fori_loop(0, steps, begin, 0)
    wo_copy.start()

    normed = rms(x_ref[...].astype(F32), g_ref[...].astype(F32).reshape(1, -1))
    lens_row = lens_v[...].reshape(1, rows).astype(F32)
    lens_col = jnp.transpose(jnp.broadcast_to(lens_row, (rows, rows)))
    lens_b[...] = lens_col
    lane = lax.broadcasted_iota(jnp.int32, (rows, 2 * dim), 1)
    low = lane < dim
    first = (lane & (dim - 1)) < dim // 2
    angles = lens_col * freq_ref[...]
    cos_t = jnp.cos(angles)
    sin_t = jnp.where(first, -jnp.sin(angles), jnp.sin(angles))

    def rope(vals):
        partner = jnp.where(first, pltpu.roll(vals, 2 * dim - dim // 2, 1), pltpu.roll(vals, dim // 2, 1))
        return vals * cos_t + partner * sin_t

    w_copies[1].wait()
    w_copies[2].wait()
    kv = lax.dot_general(normed, wkv_v[...], NT, preferred_element_type=F32)
    bkv = jnp.concatenate([bk_ref[...].astype(F32).reshape(1, dim), bv_ref[...].astype(F32).reshape(1, dim)], axis=1)
    kv = kv + bkv
    kv = jnp.where(low, rope(kv), kv).astype(BF16).astype(F32)
    kvt[...] = jnp.transpose(kv).astype(BF16)
    w_copies[0].wait()
    q_all = jnp.dot(normed, wq_v[...], preferred_element_type=F32) + bq_ref[...].astype(F32).reshape(1, -1)
    for half in range(2):
        q_half = rope(q_all[:, half * 2 * dim:(half + 1) * 2 * dim]).astype(BF16).astype(F32)
        swapped = pltpu.roll(q_half, dim, 1)
        qq[2 * half] = jnp.where(low, q_half, swapped)
        qq[2 * half + 1] = jnp.where(low, swapped, q_half)

    def body(step, carry):
        k_copy, v_copy, k_back, v_back = moves(step)
        base = pl.multiple_of(step * span, span)
        row0 = pl.multiple_of(step * (SEQ * SUB), SEQ * SUB)
        count = SEQ * SUB
        pick = (lax.broadcasted_iota(jnp.int32, (rows, count * 128), 0)
                == row0 + (lax.broadcasted_iota(jnp.int32, (rows, count * 128), 1) >> 7))
        fresh = jnp.dot(kvt[...], jnp.where(pick, 1.0, 0.0).astype(BF16), preferred_element_type=F32)
        k_copy.wait()
        v_copy.wait()
        lane_id = lax.broadcasted_iota(jnp.int32, (dim, 128), 1)
        for i in range(count):
            length = lens_s[row0 + i]
            start = pl.multiple_of((length >> 7) << 7, 128)
            hit = lane_id == (length - start)
            tile = fresh[:, i * 128:(i + 1) * 128]
            where_k = (pl.ds(base + i * dim, dim), pl.ds(start, 128))
            kbuf[where_k] = jnp.where(hit, tile[:dim], kbuf[where_k].astype(F32)).astype(BF16)
            vbuf[where_k] = jnp.where(hit, tile[dim:], vbuf[where_k].astype(F32)).astype(BF16)
        k_back.start()
        v_back.start()
        own = (lax.broadcasted_iota(jnp.int32, (SEQ, SEQ * dim), 1) // dim
               == lax.broadcasted_iota(jnp.int32, (SEQ, SEQ * dim), 0))
        slot = lax.broadcasted_iota(jnp.int32, (SEQ, slots), 1).astype(F32)
        scores = []
        for s in range(SUB):
            r0 = pl.multiple_of(row0 + s * SEQ, SEQ)
            q_blk = qq[:, pl.ds(r0, SEQ), :]
            wide = jnp.concatenate([q_blk] * (SEQ * dim // q_blk.shape[2]), axis=2)
            lhs = jnp.where(own[None], wide, 0.0).reshape(4 * SEQ, SEQ * dim).astype(BF16)
            keys = kbuf[pl.ds(base + s * SEQ * dim, SEQ * dim), :]
            scores.append(jnp.dot(lhs, keys, preferred_element_type=F32) * (dim ** -0.5))
        probs = []
        for s in range(SUB):
            r0 = pl.multiple_of(row0 + s * SEQ, SEQ)
            limit = lens_b[pl.ds(r0, SEQ), :][:, :1]
            masked = jnp.where((slot <= limit)[None], scores[s].reshape(4, SEQ, slots), -jnp.inf)
            top = jnp.max(masked, axis=-1, keepdims=True)
            weight = jnp.exp(masked - top)
            total = jnp.sum(weight, axis=-1, keepdims=True)
            probs.append((weight / total).reshape(4 * SEQ, slots).astype(BF16))
        for s in range(SUB):
            r0 = pl.multiple_of(row0 + s * SEQ, SEQ)
            vals = vbuf[pl.ds(base + s * SEQ * dim, SEQ * dim), :]
            out = lax.dot_general(probs[s], vals, NT, preferred_element_type=F32)
            out = jnp.where(own[None], out.reshape(4, SEQ, SEQ * dim), 0.0)
            width = 2 * dim
            fold = out[:, :, :width]
            for j in range(1, SEQ * dim // width):
                fold = fold + out[:, :, j * width:(j + 1) * width]
            fold = fold.reshape(4 * SEQ, width)
            fold = (fold + pltpu.roll(fold, dim, 1)).reshape(4, SEQ, width)
            low8 = lax.broadcasted_iota(jnp.int32, (SEQ, width), 1) < dim
            o_s[pl.ds(r0, SEQ), :width] = jnp.where(low8, fold[0], fold[1])
            o_s[pl.ds(r0, SEQ), width:] = jnp.where(low8, fold[2], fold[3])
        return carry

    lax.fori_loop(0, steps, body, 0)
    wo_copy.wait()
    part[...] = jnp.dot(o_s[...].astype(BF16), wo_v[...], preferred_element_type=F32).astype(BF16)

    def finish(step, carry):
        _, _, k_back, v_back = moves(step)
        k_back.wait()
        v_back.wait()
        return carry

    lax.fori_loop(0, steps, finish, 0)


def attention(x, lens, kc, vc, g, wq, bq, wk, bk, wv, bv, wo):
    rows, width = x.shape
    slots, dim = kc.shape[1], kc.shape[3]
    flat = rows * dim
    kt = jnp.transpose(kc, (0, 2, 3, 1)).reshape(flat, slots)
    vt = jnp.transpose(vc, (0, 2, 3, 1)).reshape(flat, slots)
    inv_freq = np.power(np.float64(THETA), np.arange(dim // 2) * (-2.0 / dim)).astype(np.float32)
    freq = jnp.asarray(np.tile(inv_freq, 4)[None, :])
    steps = rows // (SEQ * SUB)
    vmem = pl.BlockSpec(memory_space=pltpu.VMEM)
    hbm = pl.BlockSpec(memory_space=pl.ANY)
    dma = pltpu.SemaphoreType.DMA
    ko, vo, part = pl.pallas_call(
        attn_kernel,
        out_shape=(jax.ShapeDtypeStruct((flat, slots), BF16), jax.ShapeDtypeStruct((flat, slots), BF16),
                   jax.ShapeDtypeStruct((rows, width), BF16)),
        in_specs=[pl.BlockSpec(memory_space=pltpu.SMEM)] + [vmem] * 7 + [hbm] * 6,
        out_specs=(hbm, hbm, vmem),
        scratch_shapes=[pltpu.VMEM((flat, slots), BF16), pltpu.VMEM((flat, slots), BF16),
                        pltpu.VMEM(wq.shape, BF16), pltpu.VMEM((2 * dim, width), BF16), pltpu.VMEM(wo.shape, BF16),
                        pltpu.VMEM((rows, rows), F32), pltpu.VMEM((4, rows, 2 * dim), F32),
                        pltpu.VMEM((2 * dim, rows), BF16), pltpu.VMEM((rows, 4 * dim), F32),
                        dma((steps,)), dma((steps,)), dma((steps,)), dma((steps,)), dma((4,))],
        compiler_params=pltpu.CompilerParams(vmem_limit_bytes=48 * 1024 * 1024),
        name='attn',
    )(lens, lens, x, g, bq, bk, bv, freq, kt, vt, wq, wk.T, wv.T, wo)
    back = lambda c: jnp.transpose(c.reshape(rows, 1, dim, slots), (0, 3, 1, 2))
    return part, back(ko), back(vo)


CHUNK = 512
SLOTS = 20


def tail_kernel(part_ref, x_ref, tok_ref, gm_ref, gf_ref, wg, wu, wd, wh,
                y_out, logp_out, lse_out,
                wg_v, wu_v, wd_v, head_v, last_v, d2d, xs, xr, m_s, y_s, a_s, h_s, p_s, f_s, st_s, st_r,
                w_sem, h_sem, d_send, d_recv, x_send, x_recv, g_send, g_recv, f_send, f_recv, s_send, s_recv, y_sem):
    me = lax.axis_index('tp')
    n_tp = 2 * xs.shape[1]
    chips = n_tp // 2
    xi, core = me // 2, me % 2
    sibling = {'tp': me + 1 - 2 * core}
    rows, width = part_ref.shape
    half = rows // 2
    piece = half // chips

    w_copies = [pltpu.make_async_copy(wg, wg_v, w_sem.at[0]), pltpu.make_async_copy(wu, wu_v, w_sem.at[1]),
                pltpu.make_async_copy(wd, wd_v, w_sem.at[2])]
    for copy in w_copies:
        copy.start()
    vocab = wh.shape[0]
    full = vocab // CHUNK
    rest = vocab - full * CHUNK

    def head_copy(i):
        slot = lax.rem(i, SLOTS)
        return pltpu.make_async_copy(wh.at[pl.ds(pl.multiple_of(i * CHUNK, CHUNK), CHUNK)], head_v.at[slot], h_sem.at[slot])

    def head_begin(i, carry):
        head_copy(i).start()
        return carry

    lax.fori_loop(0, min(SLOTS, full), head_begin, 0)
    last_copy = pltpu.make_async_copy(wh.at[pl.ds(full * CHUNK, rest)], last_v, w_sem.at[3])
    last_copy.start()

    barrier = pltpu.get_barrier_semaphore()
    for k in range(1, n_tp):
        pl.semaphore_signal(barrier, inc=1, device_id={'tp': lax.rem(me + k, n_tp)}, device_id_type=MESH)
    pl.semaphore_wait(barrier, n_tp - 1)

    def rows_of(side, chip):
        return pl.ds(pl.multiple_of(side * half + chip * piece, piece), piece)

    def exchange(rnd, src, full_ref, finish):
        order = [2, 1, 3]

        def pair_copy(k):
            chip = lax.rem(xi + k, chips)
            return pltpu.make_async_remote_copy(
                src_ref=src.at[rows_of(1 - core, chip)], dst_ref=d2d.at[rnd, k],
                send_sem=d_send.at[rnd, k], recv_sem=d_recv.at[rnd, k], device_id=sibling, device_id_type=MESH)

        def ring_copy(k):
            return pltpu.make_async_remote_copy(
                src_ref=xs.at[rnd, k], dst_ref=xr.at[rnd, k], send_sem=x_send.at[rnd, k], recv_sem=x_recv.at[rnd, k],
                device_id={'tp': lax.rem(xi + k, chips) * 2 + core}, device_id_type=MESH)

        mine = rows_of(core, xi)

        def share_copy(k):
            return pltpu.make_async_remote_copy(
                src_ref=full_ref.at[mine], dst_ref=full_ref.at[mine], send_sem=g_send.at[rnd, k], recv_sem=g_recv.at[rnd, k],
                device_id={'tp': lax.rem(xi + k, chips) * 2 + core}, device_id_type=MESH)

        def forward_copy(k):
            its = rows_of(core, lax.rem(xi + chips - k, chips))
            return pltpu.make_async_remote_copy(
                src_ref=full_ref.at[its], dst_ref=full_ref.at[its], send_sem=f_send.at[rnd, k], recv_sem=f_recv.at[rnd, k],
                device_id=sibling, device_id_type=MESH)

        for k in order + [0]:
            pair_copy(k).start()
        for k in order:
            pair_copy(k).wait_recv()
            chip = lax.rem(xi + k, chips)
            xs[rnd, k] = (src[rows_of(core, chip), :].astype(F32) + d2d[rnd, k].astype(F32)).astype(BF16)
            ring_copy(k).start()
        pair_copy(0).wait_recv()
        total = src[mine, :].astype(F32) + d2d[rnd, 0].astype(F32)
        for k in (1, 3, 2):
            ring_copy(k).wait_recv()
            total = total + xr[rnd, k].astype(F32)
        full_ref[mine, :] = finish(total)
        for k in order:
            share_copy(k).start()
        forward_copy(0).start()
        for k in (1, 3, 2):
            share_copy(k).wait_recv()
            forward_copy(k).start()
        for k in range(chips):
            forward_copy(k).wait_recv()
        for k in range(chips):
            pair_copy(k).wait_send()
            forward_copy(k).wait_send()
            if k:
                ring_copy(k).wait_send()
                share_copy(k).wait_send()

    mine = rows_of(core, xi)

    def finish_attn(total):
        a = (x_ref[mine, :].astype(F32) + total).astype(BF16)
        a_s[...] = a
        return rms(a.astype(F32), gm_ref[...].astype(F32).reshape(1, -1))

    exchange(0, part_ref, m_s, finish_attn)

    w_copies[0].wait()
    w_copies[1].wait()
    ff = wg_v.shape[1]

    def gate_up(j, carry):
        cols = pl.ds(pl.multiple_of(j * 256, 256), 256)
        gate = jnp.dot(m_s[...], wg_v[:, cols], preferred_element_type=F32)
        up = jnp.dot(m_s[...], wu_v[:, cols], preferred_element_type=F32)
        h_s[:, cols] = (gate * jax.nn.sigmoid(gate) * up).astype(BF16)
        return carry

    lax.fori_loop(0, ff // 256, gate_up, 0)
    w_copies[2].wait()

    def down(j, carry):
        cols = pl.ds(pl.multiple_of(j * 512, 512), 512)
        p_s[:, cols] = jnp.dot(h_s[...], wd_v[:, cols], preferred_element_type=F32).astype(BF16)
        return carry

    lax.fori_loop(0, width // 512, down, 0)

    exchange(1, p_s, y_s, lambda total: (a_s[...].astype(F32) + total).astype(BF16))

    y_copy = pltpu.make_async_copy(y_s, y_out, y_sem)
    y_copy.start()
    gain = gf_ref[...].astype(F32).reshape(1, -1)
    f_s[...] = rms(y_s[...].astype(F32), gain)

    local_tok = tok_ref[...].reshape(1, rows) - me * vocab

    def score(weights, first_row, carry):
        top, total, target = carry
        z = lax.dot_general(weights, f_s[...], NT, preferred_element_type=F32)
        z3 = z.reshape(z.shape[0] // 8, 8, rows)
        new_top = jnp.maximum(top, jnp.max(z3, axis=0))
        total = total * jnp.exp(top - new_top) + jnp.sum(jnp.exp(z3 - new_top[None]), axis=0)
        ids = lax.broadcasted_iota(jnp.int32, z.shape, 0)
        hit = ids == (local_tok - first_row)
        target = target + jnp.sum(jnp.where(hit, z, 0.0).reshape(z3.shape), axis=0)
        return new_top, total, target

    zero = jnp.zeros((8, rows), F32)
    last_copy.wait()
    carry = score(last_v[...], full * CHUNK, (jnp.full((8, rows), -1e30, F32), zero, zero))

    def head_step(i, carry):
        head_copy(i).wait()
        slot = lax.rem(i, SLOTS)
        carry = score(head_v[slot], i * CHUNK, carry)

        @pl.when(i + SLOTS < full)
        def _():
            head_copy(i + SLOTS).start()

        return carry

    top8, total8, target8 = lax.fori_loop(0, full, head_step, carry)
    top = jnp.max(top8, axis=0, keepdims=True)
    total = jnp.sum(total8 * jnp.exp(top8 - top), axis=0, keepdims=True)
    target = jnp.sum(target8, axis=0, keepdims=True)
    st_s[...] = jnp.concatenate([top, total, target, jnp.zeros((5, rows), F32)], axis=0)

    def stat_copy(k):
        return pltpu.make_async_remote_copy(
            src_ref=st_s, dst_ref=st_r.at[k], send_sem=s_send.at[k], recv_sem=s_recv.at[k],
            device_id={'tp': lax.rem(me + k, n_tp)}, device_id_type=MESH)

    for k in range(1, n_tp):
        stat_copy(k).start()
    y_copy.wait()
    for k in range(1, n_tp):
        stat_copy(k).wait_recv()
    tops = [top] + [st_r[k, 0:1, :] for k in range(1, n_tp)]
    totals = [total] + [st_r[k, 1:2, :] for k in range(1, n_tp)]
    best = functools.reduce(jnp.maximum, tops)
    mass = sum(s * jnp.exp(t - best) for s, t in zip(totals, tops))
    hit = target + sum(st_r[k, 2:3, :] for k in range(1, n_tp))
    lse = best + jnp.log(mass)
    lse_out[...] = lse.reshape(rows)
    logp_out[...] = (hit - lse).reshape(rows)
    for k in range(1, n_tp):
        stat_copy(k).wait_send()


def tail(part, x, tok, gm, gf, wg, wu, wd, wh, n_tp):
    rows, width = x.shape
    chips = n_tp // 2
    piece = rows // n_tp
    vmem = pl.BlockSpec(memory_space=pltpu.VMEM)
    hbm = pl.BlockSpec(memory_space=pl.ANY)
    dma = pltpu.SemaphoreType.DMA
    rest = wh.shape[0] % CHUNK
    return pl.pallas_call(
        tail_kernel,
        out_shape=(jax.ShapeDtypeStruct((rows, width), BF16), jax.ShapeDtypeStruct((rows,), F32),
                   jax.ShapeDtypeStruct((rows,), F32)),
        in_specs=[vmem] * 5 + [hbm] * 4,
        out_specs=(hbm, vmem, vmem),
        scratch_shapes=[pltpu.VMEM(wg.shape, BF16), pltpu.VMEM(wu.shape, BF16), pltpu.VMEM(wd.shape, BF16),
                        pltpu.VMEM((SLOTS, CHUNK, width), BF16), pltpu.VMEM((rest, width), BF16),
                        pltpu.VMEM((2, chips, piece, width), BF16), pltpu.VMEM((2, chips, piece, width), BF16),
                        pltpu.VMEM((2, chips, piece, width), BF16),
                        pltpu.VMEM((rows, width), BF16), pltpu.VMEM((rows, width), BF16),
                        pltpu.VMEM((piece, width), BF16), pltpu.VMEM((rows, wg.shape[1]), BF16),
                        pltpu.VMEM((rows, width), BF16), pltpu.VMEM((rows, width), BF16),
                        pltpu.VMEM((8, rows), F32), pltpu.VMEM((n_tp, 8, rows), F32),
                        dma((4,)), dma((SLOTS,)),
                        dma((2, chips)), dma((2, chips)), dma((2, chips)), dma((2, chips)),
                        dma((2, chips)), dma((2, chips)), dma((2, chips)), dma((2, chips)),
                        dma((n_tp,)), dma((n_tp,)), dma],
        compiler_params=pltpu.CompilerParams(vmem_limit_bytes=67043328, collective_id=0, has_side_effects=True),
        name='tail',
    )(part, x, tok, gm, gf, wg, wu, wd, wh)


def solution(mesh):
    n_tp = mesh.shape['tp']

    def local_step(tok_hidden, seq_lens, k_cache, v_cache, next_tok, g_attn, w_q, b_q, w_k, b_k, w_v, b_v, w_o, g_mlp,
                   w_gate, w_up, w_down, g_final, w_head):
        part, k_all, v_all = attention(tok_hidden, seq_lens, k_cache, v_cache, g_attn, w_q, b_q, w_k, b_k, w_v, b_v, w_o)
        y_out, tok_logp, norm_lse = tail(part, tok_hidden, next_tok, g_mlp, g_final, w_gate, w_up, w_down, w_head, n_tp)
        return y_out, k_all, v_all, tok_logp, norm_lse

    row_spec = P('dp', None)
    vec_spec = P('dp')
    cache_spec = P('dp', None, 'tp', None)
    col_spec = P(None, 'tp')
    part_spec = P('tp')
    whole_spec = P(None)
    in_specs = (row_spec, vec_spec, cache_spec, cache_spec, vec_spec, whole_spec, col_spec, part_spec, col_spec, part_spec,
                col_spec, part_spec, P('tp', None), whole_spec, col_spec, col_spec, P('tp', None), whole_spec, P('tp', None))
    out_specs = (row_spec, cache_spec, cache_spec, vec_spec, vec_spec)
    return jax.shard_map(local_step, mesh=mesh, in_specs=in_specs, out_specs=out_specs, check_vma=False)
```

```python
import functools
import math
import jax
import jax.numpy as jnp
from jax import lax
from jax.experimental import pallas as pl
from jax.experimental.pallas import tpu as pltpu
from jax.sharding import PartitionSpec as P

THETA = 1000000.0
EPS = 1e-6
MESH = pl.DeviceIdType.MESH
NT = (((1,), (1,)), ((), ()))
F32 = jnp.float32
BF16 = jnp.bfloat16


def rms(vals_f32, gain_f32):
    inv_rms = lax.rsqrt(jnp.mean(vals_f32 * vals_f32, axis=-1, keepdims=True) + EPS)
    return (vals_f32 * inv_rms * gain_f32).astype(BF16)


VMEM_ALL = 67043328
SEQ = 8
SUB = 2


def attn_kernel(lens, x, g, bq, bk, bv, kc, vc, wq, wk, wv, wo,
                ko, vo, part, kbuf, vbuf, wq_v, wkv_v, wo_v, lens_b, qq, kvt, o_s,
                part_s, lens_s, lens_v, x_ref, g_ref, bq_ref, bk_ref, bv_ref,
                k_in, v_in, k_out, v_out, w_sem, i_sem):
    rows = x_ref.shape[0]
    dim = wk.shape[0]
    slots = kbuf.shape[1]
    span = SEQ * SUB * dim
    steps = kbuf.shape[0] // span

    small = [pltpu.make_async_copy(src, dst, i_sem.at[n]) for n, (src, dst) in enumerate(
        [(x, x_ref), (g, g_ref), (lens, lens_v), (lens, lens_s), (bq, bq_ref), (bk, bk_ref), (bv, bv_ref)])]
    for copy in small:
        copy.start()
    w_copies = [pltpu.make_async_copy(wq, wq_v, w_sem.at[0]),
                pltpu.make_async_copy(wk, wkv_v.at[pl.ds(0, dim)], w_sem.at[1]),
                pltpu.make_async_copy(wv, wkv_v.at[pl.ds(dim, dim)], w_sem.at[2])]
    wo_copy = pltpu.make_async_copy(wo, wo_v, w_sem.at[3])
    for copy in w_copies:
        copy.start()

    def moves(step):
        here = pl.ds(pl.multiple_of(step * span, span), span)
        return (pltpu.make_async_copy(kc.at[here], kbuf.at[here], k_in.at[step]),
                pltpu.make_async_copy(vc.at[here], vbuf.at[here], v_in.at[step]),
                pltpu.make_async_copy(kbuf.at[here], ko.at[here], k_out.at[step]),
                pltpu.make_async_copy(vbuf.at[here], vo.at[here], v_out.at[step]))

    def begin(step, carry):
        k_copy, v_copy, _, _ = moves(step)
        k_copy.start()
        v_copy.start()
        return carry

    lax.fori_loop(0, steps, begin, 0)
    wo_copy.start()

    for copy in small:
        copy.wait()
    normed = rms(x_ref[...].astype(F32), g_ref[...].astype(F32).reshape(1, -1))
    lens_row = lens_v[...].reshape(1, rows).astype(F32)
    lens_col = jnp.transpose(jnp.broadcast_to(lens_row, (rows, rows)))
    lens_b[...] = lens_col
    lane = lax.broadcasted_iota(jnp.int32, (rows, 2 * dim), 1)
    low = lane < dim
    first = (lane & (dim - 1)) < dim // 2
    power = (lane & (dim // 2 - 1)).astype(F32) * (-2.0 / dim)
    angles = lens_col * jnp.exp(power * math.log(THETA))
    cos_t = jnp.cos(angles)
    sin_t = jnp.where(first, -jnp.sin(angles), jnp.sin(angles))

    def rope(vals):
        partner = jnp.where(first, pltpu.roll(vals, 2 * dim - dim // 2, 1), pltpu.roll(vals, dim // 2, 1))
        return vals * cos_t + partner * sin_t

    w_copies[1].wait()
    w_copies[2].wait()
    kv = lax.dot_general(normed, wkv_v[...], NT, preferred_element_type=F32)
    bkv = jnp.concatenate([bk_ref[...].astype(F32).reshape(1, dim), bv_ref[...].astype(F32).reshape(1, dim)], axis=1)
    kv = kv + bkv
    kv = jnp.where(low, rope(kv), kv).astype(BF16).astype(F32)
    kvt[...] = jnp.transpose(kv).astype(BF16)
    w_copies[0].wait()
    q_all = jnp.dot(normed, wq_v[...], preferred_element_type=F32) + bq_ref[...].astype(F32).reshape(1, -1)
    for half in range(2):
        q_half = rope(q_all[:, half * 2 * dim:(half + 1) * 2 * dim]).astype(BF16).astype(F32)
        swapped = pltpu.roll(q_half, dim, 1)
        qq[2 * half] = jnp.where(low, q_half, swapped)
        qq[2 * half + 1] = jnp.where(low, swapped, q_half)

    def body(step, carry):
        k_copy, v_copy, k_back, v_back = moves(step)
        base = pl.multiple_of(step * span, span)
        row0 = pl.multiple_of(step * (SEQ * SUB), SEQ * SUB)
        count = SEQ * SUB
        pick = (lax.broadcasted_iota(jnp.int32, (rows, count * 128), 0)
                == row0 + (lax.broadcasted_iota(jnp.int32, (rows, count * 128), 1) >> 7))
        fresh = jnp.dot(kvt[...], jnp.where(pick, 1.0, 0.0).astype(BF16), preferred_element_type=F32)
        k_copy.wait()
        v_copy.wait()
        lane_id = lax.broadcasted_iota(jnp.int32, (dim, 128), 1)
        for i in range(count):
            length = lens_s[row0 + i]
            start = pl.multiple_of((length >> 7) << 7, 128)
            hit = lane_id == (length - start)
            tile = fresh[:, i * 128:(i + 1) * 128]
            where_k = (pl.ds(base + i * dim, dim), pl.ds(start, 128))
            kbuf[where_k] = jnp.where(hit, tile[:dim], kbuf[where_k].astype(F32)).astype(BF16)
            vbuf[where_k] = jnp.where(hit, tile[dim:], vbuf[where_k].astype(F32)).astype(BF16)
        k_back.start()
        v_back.start()
        own = (lax.broadcasted_iota(jnp.int32, (SEQ, SEQ * dim), 1) // dim
               == lax.broadcasted_iota(jnp.int32, (SEQ, SEQ * dim), 0))
        slot = lax.broadcasted_iota(jnp.int32, (SEQ, slots), 1).astype(F32)
        scores = []
        for s in range(SUB):
            r0 = pl.multiple_of(row0 + s * SEQ, SEQ)
            q_blk = qq[:, pl.ds(r0, SEQ), :]
            wide = jnp.concatenate([q_blk] * (SEQ * dim // q_blk.shape[2]), axis=2)
            lhs = jnp.where(own[None], wide, 0.0).reshape(4 * SEQ, SEQ * dim).astype(BF16)
            keys = kbuf[pl.ds(base + s * SEQ * dim, SEQ * dim), :]
            scores.append(jnp.dot(lhs, keys, preferred_element_type=F32) * (dim ** -0.5))
        probs = []
        for s in range(SUB):
            r0 = pl.multiple_of(row0 + s * SEQ, SEQ)
            limit = lens_b[pl.ds(r0, SEQ), :][:, :1]
            masked = jnp.where((slot <= limit)[None], scores[s].reshape(4, SEQ, slots), -jnp.inf)
            top = jnp.max(masked, axis=-1, keepdims=True)
            weight = jnp.exp(masked - top)
            total = jnp.sum(weight, axis=-1, keepdims=True)
            probs.append((weight / total).reshape(4 * SEQ, slots).astype(BF16))
        for s in range(SUB):
            r0 = pl.multiple_of(row0 + s * SEQ, SEQ)
            vals = vbuf[pl.ds(base + s * SEQ * dim, SEQ * dim), :]
            out = lax.dot_general(probs[s], vals, NT, preferred_element_type=F32)
            out = jnp.where(own[None], out.reshape(4, SEQ, SEQ * dim), 0.0)
            width = 2 * dim
            fold = out[:, :, :width]
            for j in range(1, SEQ * dim // width):
                fold = fold + out[:, :, j * width:(j + 1) * width]
            fold = fold.reshape(4 * SEQ, width)
            fold = (fold + pltpu.roll(fold, dim, 1)).reshape(4, SEQ, width)
            low8 = lax.broadcasted_iota(jnp.int32, (SEQ, width), 1) < dim
            o_s[pl.ds(r0, SEQ), :width] = jnp.where(low8, fold[0], fold[1])
            o_s[pl.ds(r0, SEQ), width:] = jnp.where(low8, fold[2], fold[3])
        return carry

    lax.fori_loop(0, steps, body, 0)
    wo_copy.wait()
    part_s[...] = jnp.dot(o_s[...].astype(BF16), wo_v[...], preferred_element_type=F32).astype(BF16)
    part_copy = pltpu.make_async_copy(part_s, part, w_sem.at[4])
    part_copy.start()

    def finish(step, carry):
        _, _, k_back, v_back = moves(step)
        k_back.wait()
        v_back.wait()
        return carry

    lax.fori_loop(0, steps, finish, 0)
    part_copy.wait()


def attention(x, lens, kc, vc, g, wq, bq, wk, bk, wv, bv, wo):
    rows, width = x.shape
    slots, dim = kc.shape[1], kc.shape[3]
    flat = rows * dim
    kt = jnp.transpose(kc, (0, 2, 3, 1)).reshape(flat, slots)
    vt = jnp.transpose(vc, (0, 2, 3, 1)).reshape(flat, slots)
    steps = rows // (SEQ * SUB)
    vmem = pl.BlockSpec(memory_space=pltpu.VMEM)
    hbm = pl.BlockSpec(memory_space=pltpu.HBM)
    dma = pltpu.SemaphoreType.DMA
    ko, vo, part = pl.pallas_call(
        attn_kernel,
        out_shape=(jax.ShapeDtypeStruct((flat, slots), BF16), jax.ShapeDtypeStruct((flat, slots), BF16),
                   jax.ShapeDtypeStruct((rows, width), BF16)),
        in_specs=[hbm] * 12,
        out_specs=(hbm, hbm, hbm),
        scratch_shapes=[pltpu.VMEM((flat, slots), BF16), pltpu.VMEM((flat, slots), BF16),
                        pltpu.VMEM(wq.shape, BF16), pltpu.VMEM((2 * dim, width), BF16), pltpu.VMEM(wo.shape, BF16),
                        pltpu.VMEM((rows, rows), F32), pltpu.VMEM((4, rows, 2 * dim), F32),
                        pltpu.VMEM((2 * dim, rows), BF16), pltpu.VMEM((rows, 4 * dim), F32),
                        pltpu.VMEM(x.shape, BF16), pltpu.SMEM((rows,), jnp.int32), pltpu.VMEM((rows,), jnp.int32), pltpu.VMEM(x.shape, BF16),
                        pltpu.VMEM(g.shape, BF16), pltpu.VMEM(bq.shape, BF16), pltpu.VMEM(bk.shape, BF16),
                        pltpu.VMEM(bv.shape, BF16),
                        dma((steps,)), dma((steps,)), dma((steps,)), dma((steps,)), dma((5,)), dma((7,))],
        compiler_params=pltpu.CompilerParams(vmem_limit_bytes=VMEM_ALL),
        name='attn',
    )(lens, x, g, bq, bk, bv, kt, vt, wq, wk.T, wv.T, wo)
    back = lambda c: jnp.transpose(c.reshape(rows, 1, dim, slots), (0, 3, 1, 2))
    return part, back(ko), back(vo)


CHUNK = 512
SLOTS = 26
MLP_SLOTS = 6
EARLY = 14
BLOCK = 256
CHEW = ((0, 7, 3), (0, 5, 5))
LOW = -1e30
GROUP = 4


def tail_kernel(part, x, tok, gm, gf, wg, wu, wd, wh,
                y_s, stats,
                buf, last_v, d2d, xs, xr, m_s, a_s, h_s, p_s, f_s, acc, tok_c, st_s, st_r,
                part_ref, x_v, tok_v, gm_v, gf_v,
                w_sem, h_sem, d_send, d_recv, x_send, x_recv, g_send, g_recv, f_send, f_recv, s_send, s_recv):
    me = lax.axis_index('tp')
    n_tp = 2 * xs.shape[1]
    chips = n_tp // 2
    xi, core = me // 2, me % 2
    sibling = {'tp': me + 1 - 2 * core}
    rows, width = part.shape
    half = rows // 2
    piece = half // chips
    ff = wg.shape[1]
    vocab = wh.shape[0]
    full = vocab // CHUNK
    rest = vocab - full * CHUNK

    def rows_of(side, chip):
        return pl.ds(pl.multiple_of(side * half + chip * piece, piece), piece)

    mine = rows_of(core, xi)

    small = [pltpu.make_async_copy(x.at[mine], x_v, w_sem.at[0]), pltpu.make_async_copy(tok, tok_v, w_sem.at[1]),
             pltpu.make_async_copy(gm, gm_v, w_sem.at[2]), pltpu.make_async_copy(gf, gf_v, w_sem.at[3]),
             pltpu.make_async_copy(part, part_ref, w_sem.at[15])]
    last_copy = pltpu.make_async_copy(wh.at[pl.ds(full * CHUNK, rest)], last_v.at[pl.ds(0, rest)], w_sem.at[4])
    mlp_copies = []
    for n, w in enumerate((wg, wu)):
        for kb in range(width // CHUNK):
            mlp_copies.append(pltpu.make_async_copy(
                w.at[pl.ds(kb * CHUNK, CHUNK)], buf.at[2 * n + kb // 2, :, pl.ds((kb % 2) * ff, ff)],
                w_sem.at[5 + 4 * n + kb]))
    for kb in range(ff // CHUNK):
        mlp_copies.append(pltpu.make_async_copy(wd.at[pl.ds(kb * CHUNK, CHUNK)], buf.at[4 + kb], w_sem.at[13 + kb]))

    def slot_of(i):
        return lax.rem(i + MLP_SLOTS, SLOTS)

    def head_copy(i):
        return pltpu.make_async_copy(wh.at[pl.ds(pl.multiple_of(i * CHUNK, CHUNK), CHUNK)], buf.at[slot_of(i)],
                                     h_sem.at[slot_of(i)])

    def head_begin(i, carry):
        head_copy(i).start()
        return carry

    for copy in small:
        copy.start()
    lax.fori_loop(0, EARLY, head_begin, 0)
    for copy in mlp_copies:
        copy.start()
    lax.fori_loop(EARLY, SLOTS - MLP_SLOTS, head_begin, 0)
    last_copy.start()

    barrier = pltpu.get_barrier_semaphore()
    for k in range(1, n_tp):
        pl.semaphore_signal(barrier, inc=1, device_id={'tp': lax.rem(me + k, n_tp)}, device_id_type=MESH)

    last_v[pl.ds(rest, last_v.shape[0] - rest), :] = jnp.zeros((last_v.shape[0] - rest, width), BF16)
    acc[0] = jnp.full((rows, 128), LOW, F32)
    acc[1] = jnp.zeros((rows, 128), F32)
    acc[2] = jnp.zeros((rows, 128), F32)
    for copy in small:
        copy.wait()
    tok_row = (tok_v[...].reshape(1, rows) - me * vocab).astype(F32)
    tok_row = jnp.where((tok_row >= 0) & (tok_row < vocab), tok_row, -float(2 * vocab))
    tok_c[...] = jnp.transpose(jnp.broadcast_to(tok_row, (rows, rows))).astype(jnp.int32)

    pl.semaphore_wait(barrier, n_tp - 1)

    turned = [0]

    def chew(count):
        first = turned[0]
        turned[0] += count

        def one(i, carry):
            head_copy(i).wait()
            slot = slot_of(i)

            def strip(c, inner):
                cols = pl.ds(pl.multiple_of(c * BLOCK, BLOCK), BLOCK)
                for r in range(CHUNK // BLOCK):
                    band = pl.ds(r * BLOCK, BLOCK)
                    buf[slot, band, cols] = jnp.transpose(buf[slot, band, cols])
                return inner

            lax.fori_loop(0, width // BLOCK, strip, 0)
            return carry

        if count:
            lax.fori_loop(first, first + count, one, 0)

    def exchange(rnd, src, full_ref, finish):
        order = [2, 1, 3]

        def pair_copy(k):
            chip = lax.rem(xi + k, chips)
            return pltpu.make_async_remote_copy(
                src_ref=src.at[rows_of(1 - core, chip)], dst_ref=d2d.at[rnd, k],
                send_sem=d_send.at[rnd, k], recv_sem=d_recv.at[rnd, k], device_id=sibling, device_id_type=MESH)

        def ring_copy(k):
            return pltpu.make_async_remote_copy(
                src_ref=xs.at[rnd, k], dst_ref=xr.at[rnd, k], send_sem=x_send.at[rnd, k], recv_sem=x_recv.at[rnd, k],
                device_id={'tp': lax.rem(xi + k, chips) * 2 + core}, device_id_type=MESH)

        def share_copy(k):
            return pltpu.make_async_remote_copy(
                src_ref=full_ref.at[mine], dst_ref=full_ref.at[mine], send_sem=g_send.at[rnd, k], recv_sem=g_recv.at[rnd, k],
                device_id={'tp': lax.rem(xi + k, chips) * 2 + core}, device_id_type=MESH)

        def forward_copy(k):
            its = rows_of(core, lax.rem(xi + chips - k, chips))
            return pltpu.make_async_remote_copy(
                src_ref=full_ref.at[its], dst_ref=full_ref.at[its], send_sem=f_send.at[rnd, k], recv_sem=f_recv.at[rnd, k],
                device_id=sibling, device_id_type=MESH)

        for k in order + [0]:
            pair_copy(k).start()
        chew(CHEW[rnd][0])
        for k in order:
            pair_copy(k).wait_recv()
            chip = lax.rem(xi + k, chips)
            xs[rnd, k] = (src[rows_of(core, chip), :].astype(F32) + d2d[rnd, k].astype(F32)).astype(BF16)
            ring_copy(k).start()
        pair_copy(0).wait_recv()
        chew(CHEW[rnd][1])
        total = src[mine, :].astype(F32) + d2d[rnd, 0].astype(F32)
        for k in (1, 3, 2):
            ring_copy(k).wait_recv()
            total = total + xr[rnd, k].astype(F32)
        full_ref[mine, :] = finish(total)
        for k in order:
            share_copy(k).start()
        forward_copy(0).start()
        chew(CHEW[rnd][2])
        for k in (1, 3, 2):
            share_copy(k).wait_recv()
            forward_copy(k).start()
        for k in range(chips):
            forward_copy(k).wait_recv()
        for k in range(chips):
            pair_copy(k).wait_send()
            forward_copy(k).wait_send()
            if k:
                ring_copy(k).wait_send()
                share_copy(k).wait_send()

    def finish_attn(total):
        a = (x_v[...].astype(F32) + total).astype(BF16)
        a_s[...] = a
        return rms(a.astype(F32), gm_v[...].astype(F32).reshape(1, -1))

    exchange(0, part_ref, m_s, finish_attn)

    for copy in mlp_copies:
        copy.wait()

    def gate_up(j, carry):
        def product(n):
            out = None
            for kb in range(width // CHUNK):
                cols = pl.ds(pl.multiple_of((kb % 2) * ff + j * BLOCK, BLOCK), BLOCK)
                term = jnp.dot(m_s[:, kb * CHUNK:(kb + 1) * CHUNK], buf[2 * n + kb // 2, :, cols], preferred_element_type=F32)
                out = term if out is None else out + term
            return out

        gate = product(0)
        up = product(1)
        h_s[:, pl.ds(pl.multiple_of(j * BLOCK, BLOCK), BLOCK)] = (gate * jax.nn.sigmoid(gate) * up).astype(BF16)
        return carry

    lax.fori_loop(0, ff // BLOCK, gate_up, 0)

    def down(j, carry):
        cols = pl.ds(pl.multiple_of(j * CHUNK, CHUNK), CHUNK)
        out = jnp.dot(h_s[:, :CHUNK], buf[4, :, cols], preferred_element_type=F32)
        out = out + jnp.dot(h_s[:, CHUNK:], buf[5, :, cols], preferred_element_type=F32)
        p_s[:, cols] = out.astype(BF16)
        return carry

    lax.fori_loop(0, width // CHUNK, down, 0)
    lax.fori_loop(SLOTS - MLP_SLOTS, SLOTS, head_begin, 0)

    exchange(1, p_s, y_s, lambda total: (a_s[...].astype(F32) + total).astype(BF16))

    f_s[...] = rms(y_s[...].astype(F32), gf_v[...].astype(F32).reshape(1, -1))

    lane = lax.broadcasted_iota(jnp.int32, (rows, 128), 1)

    def fold(scores, first_row):
        parts = [scores[:, j * 128:(j + 1) * 128] for j in range(scores.shape[1] // 128)]
        old = acc[0]
        top = functools.reduce(jnp.maximum, parts, old)
        total = acc[1] * jnp.exp(old - top)
        target = acc[2]
        place = tok_c[...] - first_row
        for j, part in enumerate(parts):
            total = total + jnp.exp(part - top)
            target = target + jnp.where(place == lane + j * 128, part, 0.0)
        acc[0] = top
        acc[1] = total
        acc[2] = target

    def product(i, r, turned_form):
        band = pl.ds(r * BLOCK, BLOCK)
        slot = slot_of(i)
        if not turned_form:
            return lax.dot_general(f_s[...], buf[slot, band, :], NT, preferred_element_type=F32)
        out = None
        for c in range(width // BLOCK):
            term = jnp.dot(f_s[:, c * BLOCK:(c + 1) * BLOCK], buf[slot, band, c * BLOCK:(c + 1) * BLOCK],
                           preferred_element_type=F32)
            out = term if out is None else out + term
        return out

    def refill(i):
        @pl.when(i + SLOTS < full)
        def _():
            head_copy(i + SLOTS).start()

    def group(first, size, turned_form):
        def run(n, carry):
            base = first + n * size
            if not turned_form:
                for u in range(size):
                    head_copy(base + u).wait()
            for u in range(size):
                scores = [product(base + u, r, turned_form) for r in range(CHUNK // BLOCK)]
                fold(jnp.concatenate(scores, axis=1), (base + u) * CHUNK)
            for u in range(size):
                refill(base + u)
            return carry

        return run

    def sweep(first, count, turned_form):
        size = min(GROUP, count) if turned_form else 1
        if count:
            lax.fori_loop(0, count // size, group(first, size, turned_form), 0)
            if count % size:
                lax.fori_loop(0, 1, group(first + count // size * size, count % size, turned_form), 0)

    sweep(0, turned[0], True)
    sweep(turned[0], full - turned[0], False)
    last_copy.wait()
    out = lax.dot_general(f_s[...], last_v[...], NT, preferred_element_type=F32)
    ids = lax.broadcasted_iota(jnp.int32, out.shape, 1)
    fold(jnp.where(ids < rest, out, LOW), full * CHUNK)

    tops8 = jnp.transpose(acc[0])
    top = jnp.max(tops8, axis=0, keepdims=True)
    total = jnp.sum(jnp.transpose(acc[1]) * jnp.exp(tops8 - top), axis=0, keepdims=True)
    target = jnp.sum(jnp.transpose(acc[2]), axis=0, keepdims=True)
    st_s[...] = jnp.concatenate([top, total, target, jnp.zeros((5, rows), F32)], axis=0)

    def stat_copy(k):
        return pltpu.make_async_remote_copy(
            src_ref=st_s, dst_ref=st_r.at[k], send_sem=s_send.at[k], recv_sem=s_recv.at[k],
            device_id={'tp': lax.rem(me + k, n_tp)}, device_id_type=MESH)

    for k in range(1, n_tp):
        stat_copy(k).start()
    for k in range(1, n_tp):
        stat_copy(k).wait_recv()
    tops = [top] + [st_r[k, 0:1, :] for k in range(1, n_tp)]
    totals = [total] + [st_r[k, 1:2, :] for k in range(1, n_tp)]
    best = functools.reduce(jnp.maximum, tops)
    mass = sum(s * jnp.exp(t - best) for s, t in zip(totals, tops))
    hit = target + sum(st_r[k, 2:3, :] for k in range(1, n_tp))
    lse = best + jnp.log(mass)
    stats[...] = jnp.concatenate([hit - lse, lse, jnp.zeros((6, rows), F32)], axis=0)
    for k in range(1, n_tp):
        stat_copy(k).wait_send()


def tail(part, x, tok, gm, gf, wg, wu, wd, wh, n_tp):
    rows, width = x.shape
    chips = n_tp // 2
    piece = rows // n_tp
    vmem = pl.BlockSpec(memory_space=pltpu.VMEM)
    hbm = pl.BlockSpec(memory_space=pltpu.HBM)
    dma = pltpu.SemaphoreType.DMA
    rest = wh.shape[0] % CHUNK
    return pl.pallas_call(
        tail_kernel,
        out_shape=(jax.ShapeDtypeStruct((rows, width), BF16), jax.ShapeDtypeStruct((8, rows), F32)),
        in_specs=[hbm] * 9,
        out_specs=(vmem, vmem),
        scratch_shapes=[pltpu.VMEM((SLOTS, CHUNK, width), BF16), pltpu.VMEM((-(-rest // BLOCK) * BLOCK, width), BF16),
                        pltpu.VMEM((2, chips, piece, width), BF16), pltpu.VMEM((2, chips, piece, width), BF16),
                        pltpu.VMEM((2, chips, piece, width), BF16),
                        pltpu.VMEM((rows, width), BF16), pltpu.VMEM((piece, width), BF16),
                        pltpu.VMEM((rows, wg.shape[1]), BF16),
                        pltpu.VMEM((rows, width), BF16), pltpu.VMEM((rows, width), BF16),
                        pltpu.VMEM((3, rows, 128), F32), pltpu.VMEM((rows, rows), jnp.int32),
                        pltpu.VMEM((8, rows), F32), pltpu.VMEM((n_tp, 8, rows), F32),
                        pltpu.VMEM((rows, width), BF16), pltpu.VMEM((piece, width), BF16), pltpu.VMEM((rows,), jnp.int32),
                        pltpu.VMEM(gm.shape, BF16), pltpu.VMEM(gf.shape, BF16),
                        dma((16,)), dma((SLOTS,)),
                        dma((2, chips)), dma((2, chips)), dma((2, chips)), dma((2, chips)),
                        dma((2, chips)), dma((2, chips)), dma((2, chips)), dma((2, chips)),
                        dma((n_tp,)), dma((n_tp,))],
        compiler_params=pltpu.CompilerParams(vmem_limit_bytes=VMEM_TAIL, collective_id=0, has_side_effects=True),
        name='tail',
    )(part, x, tok, gm, gf, wg, wu, wd, wh)


VMEM_TAIL = VMEM_ALL


def give_kernel(y, stats, y_out, logp_out, lse_out, sem):
    copy = pltpu.make_async_copy(y, y_out, sem)
    copy.start()
    logp_out[...] = stats[0:1, :].reshape(stats.shape[1])
    lse_out[...] = stats[1:2, :].reshape(stats.shape[1])
    copy.wait()


def give(y, stats):
    rows = y.shape[0]
    vmem = pl.BlockSpec(memory_space=pltpu.VMEM)
    return pl.pallas_call(
        give_kernel,
        out_shape=(jax.ShapeDtypeStruct(y.shape, BF16), jax.ShapeDtypeStruct((rows,), F32), jax.ShapeDtypeStruct((rows,), F32)),
        in_specs=[vmem, vmem],
        out_specs=(pl.BlockSpec(memory_space=pltpu.HBM), vmem, vmem),
        scratch_shapes=[pltpu.SemaphoreType.DMA],
        compiler_params=pltpu.CompilerParams(vmem_limit_bytes=VMEM_TAIL),
        name='give',
    )(y, stats)


def solution(mesh):
    n_tp = mesh.shape['tp']

    def local_step(tok_hidden, seq_lens, k_cache, v_cache, next_tok, g_attn, w_q, b_q, w_k, b_k, w_v, b_v, w_o, g_mlp,
                   w_gate, w_up, w_down, g_final, w_head):
        part, k_all, v_all = attention(tok_hidden, seq_lens, k_cache, v_cache, g_attn, w_q, b_q, w_k, b_k, w_v, b_v, w_o)
        y_all, stats = tail(part, tok_hidden, next_tok, g_mlp, g_final, w_gate, w_up, w_down, w_head, n_tp)
        y_out, tok_logp, norm_lse = give(y_all, stats)
        return y_out, k_all, v_all, tok_logp, norm_lse

    row_spec = P('dp', None)
    vec_spec = P('dp')
    cache_spec = P('dp', None, 'tp', None)
    col_spec = P(None, 'tp')
    part_spec = P('tp')
    whole_spec = P(None)
    in_specs = (row_spec, vec_spec, cache_spec, cache_spec, vec_spec, whole_spec, col_spec, part_spec, col_spec, part_spec,
                col_spec, part_spec, P('tp', None), whole_spec, col_spec, col_spec, P('tp', None), whole_spec, P('tp', None))
    out_specs = (row_spec, cache_spec, cache_spec, vec_spec, vec_spec)
    return jax.shard_map(local_step, mesh=mesh, in_specs=in_specs, out_specs=out_specs, check_vma=False)
```

```python
import functools
import math
import jax
import jax.numpy as jnp
from jax import lax
from jax.experimental import pallas as pl
from jax.experimental.pallas import tpu as pltpu
from jax.sharding import PartitionSpec as P

THETA = 1000000.0
EPS = 1e-6
MESH = pl.DeviceIdType.MESH
NT = (((1,), (1,)), ((), ()))
F32 = jnp.float32
BF16 = jnp.bfloat16


def rms(vals_f32, gain_f32):
    inv_rms = lax.rsqrt(jnp.mean(vals_f32 * vals_f32, axis=-1, keepdims=True) + EPS)
    return (vals_f32 * inv_rms * gain_f32).astype(BF16)


VMEM_ALL = 67043328
SEQ = 8
SUB = 2


def attn_kernel(lens, x, g, bq, bk, bv, kc, vc, wq, wk, wv, wo,
                ko, vo, part, kbuf, vbuf, wq_v, wkv_v, wo_v, lens_b, qq, kvt, o_s,
                part_s, lens_s, lens_v, x_ref, g_ref, bq_ref, bk_ref, bv_ref,
                k_in, v_in, k_out, v_out, w_sem, i_sem):
    rows = x_ref.shape[0]
    dim = wk.shape[0]
    slots = kbuf.shape[1]
    span = SEQ * SUB * dim
    steps = kbuf.shape[0] // span

    small = [pltpu.make_async_copy(src, dst, i_sem.at[n]) for n, (src, dst) in enumerate(
        [(x, x_ref), (g, g_ref), (lens, lens_v), (lens, lens_s), (bq, bq_ref), (bk, bk_ref), (bv, bv_ref)])]
    for copy in small:
        copy.start()
    w_copies = [pltpu.make_async_copy(wq, wq_v, w_sem.at[0]),
                pltpu.make_async_copy(wk, wkv_v.at[pl.ds(0, dim)], w_sem.at[1]),
                pltpu.make_async_copy(wv, wkv_v.at[pl.ds(dim, dim)], w_sem.at[2])]
    wo_copy = pltpu.make_async_copy(wo, wo_v, w_sem.at[3])
    for copy in w_copies:
        copy.start()

    def moves(step):
        here = pl.ds(pl.multiple_of(step * span, span), span)
        return (pltpu.make_async_copy(kc.at[here], kbuf.at[here], k_in.at[step]),
                pltpu.make_async_copy(vc.at[here], vbuf.at[here], v_in.at[step]),
                pltpu.make_async_copy(kbuf.at[here], ko.at[here], k_out.at[step]),
                pltpu.make_async_copy(vbuf.at[here], vo.at[here], v_out.at[step]))

    def begin(step, carry):
        k_copy, v_copy, _, _ = moves(step)
        k_copy.start()
        v_copy.start()
        return carry

    lax.fori_loop(0, steps, begin, 0)
    wo_copy.start()

    for copy in small:
        copy.wait()
    normed = rms(x_ref[...].astype(F32), g_ref[...].astype(F32).reshape(1, -1))
    lens_row = lens_v[...].reshape(1, rows).astype(F32)
    lens_col = jnp.transpose(jnp.broadcast_to(lens_row, (rows, rows)))
    lens_b[...] = lens_col
    lane = lax.broadcasted_iota(jnp.int32, (rows, 2 * dim), 1)
    low = lane < dim
    first = (lane & (dim - 1)) < dim // 2
    power = (lane & (dim // 2 - 1)).astype(F32) * (-2.0 / dim)
    angles = lens_col * jnp.exp(power * math.log(THETA))
    cos_t = jnp.cos(angles)
    sin_t = jnp.where(first, -jnp.sin(angles), jnp.sin(angles))

    def rope(vals):
        partner = jnp.where(first, pltpu.roll(vals, 2 * dim - dim // 2, 1), pltpu.roll(vals, dim // 2, 1))
        return vals * cos_t + partner * sin_t

    w_copies[1].wait()
    w_copies[2].wait()
    kv = lax.dot_general(normed, wkv_v[...], NT, preferred_element_type=F32)
    bkv = jnp.concatenate([bk_ref[...].astype(F32).reshape(1, dim), bv_ref[...].astype(F32).reshape(1, dim)], axis=1)
    kv = kv + bkv
    kv = jnp.where(low, rope(kv), kv).astype(BF16).astype(F32)
    kvt[...] = jnp.transpose(kv).astype(BF16)
    w_copies[0].wait()
    q_all = jnp.dot(normed, wq_v[...], preferred_element_type=F32) + bq_ref[...].astype(F32).reshape(1, -1)
    for half in range(2):
        q_half = rope(q_all[:, half * 2 * dim:(half + 1) * 2 * dim]).astype(BF16).astype(F32)
        swapped = pltpu.roll(q_half, dim, 1)
        qq[2 * half] = jnp.where(low, q_half, swapped)
        qq[2 * half + 1] = jnp.where(low, swapped, q_half)

    def body(step, carry):
        k_copy, v_copy, k_back, v_back = moves(step)
        base = pl.multiple_of(step * span, span)
        row0 = pl.multiple_of(step * (SEQ * SUB), SEQ * SUB)
        count = SEQ * SUB
        pick = (lax.broadcasted_iota(jnp.int32, (rows, count * 128), 0)
                == row0 + (lax.broadcasted_iota(jnp.int32, (rows, count * 128), 1) >> 7))
        fresh = jnp.dot(kvt[...], jnp.where(pick, 1.0, 0.0).astype(BF16), preferred_element_type=F32)
        k_copy.wait()
        v_copy.wait()
        lane_id = lax.broadcasted_iota(jnp.int32, (dim, 128), 1)
        for i in range(count):
            length = lens_s[row0 + i]
            start = pl.multiple_of((length >> 7) << 7, 128)
            hit = lane_id == (length - start)
            tile = fresh[:, i * 128:(i + 1) * 128]
            where_k = (pl.ds(base + i * dim, dim), pl.ds(start, 128))
            kbuf[where_k] = jnp.where(hit, tile[:dim], kbuf[where_k].astype(F32)).astype(BF16)
            vbuf[where_k] = jnp.where(hit, tile[dim:], vbuf[where_k].astype(F32)).astype(BF16)
        k_back.start()
        v_back.start()
        own = (lax.broadcasted_iota(jnp.int32, (SEQ, SEQ * dim), 1) // dim
               == lax.broadcasted_iota(jnp.int32, (SEQ, SEQ * dim), 0))
        slot = lax.broadcasted_iota(jnp.int32, (SEQ, slots), 1).astype(F32)
        scores = []
        for s in range(SUB):
            r0 = pl.multiple_of(row0 + s * SEQ, SEQ)
            q_blk = qq[:, pl.ds(r0, SEQ), :]
            wide = jnp.concatenate([q_blk] * (SEQ * dim // q_blk.shape[2]), axis=2)
            lhs = jnp.where(own[None], wide, 0.0).reshape(4 * SEQ, SEQ * dim).astype(BF16)
            keys = kbuf[pl.ds(base + s * SEQ * dim, SEQ * dim), :]
            scores.append(jnp.dot(lhs, keys, preferred_element_type=F32) * (dim ** -0.5))
        probs = []
        for s in range(SUB):
            r0 = pl.multiple_of(row0 + s * SEQ, SEQ)
            limit = lens_b[pl.ds(r0, SEQ), :][:, :1]
            masked = jnp.where((slot <= limit)[None], scores[s].reshape(4, SEQ, slots), -jnp.inf)
            top = jnp.max(masked, axis=-1, keepdims=True)
            weight = jnp.exp(masked - top)
            total = jnp.sum(weight, axis=-1, keepdims=True)
            probs.append((weight / total).reshape(4 * SEQ, slots).astype(BF16))
        for s in range(SUB):
            r0 = pl.multiple_of(row0 + s * SEQ, SEQ)
            vals = vbuf[pl.ds(base + s * SEQ * dim, SEQ * dim), :]
            out = lax.dot_general(probs[s], vals, NT, preferred_element_type=F32)
            out = jnp.where(own[None], out.reshape(4, SEQ, SEQ * dim), 0.0)
            width = 2 * dim
            fold = out[:, :, :width]
            for j in range(1, SEQ * dim // width):
                fold = fold + out[:, :, j * width:(j + 1) * width]
            fold = fold.reshape(4 * SEQ, width)
            fold = (fold + pltpu.roll(fold, dim, 1)).reshape(4, SEQ, width)
            low8 = lax.broadcasted_iota(jnp.int32, (SEQ, width), 1) < dim
            o_s[pl.ds(r0, SEQ), :width] = jnp.where(low8, fold[0], fold[1])
            o_s[pl.ds(r0, SEQ), width:] = jnp.where(low8, fold[2], fold[3])
        return carry

    lax.fori_loop(0, steps, body, 0)
    wo_copy.wait()
    part_s[...] = jnp.dot(o_s[...].astype(BF16), wo_v[...], preferred_element_type=F32).astype(BF16)
    part_copy = pltpu.make_async_copy(part_s, part, w_sem.at[4])
    part_copy.start()

    def finish(step, carry):
        _, _, k_back, v_back = moves(step)
        k_back.wait()
        v_back.wait()
        return carry

    lax.fori_loop(0, steps, finish, 0)
    part_copy.wait()


def attention(x, lens, kc, vc, g, wq, bq, wk, bk, wv, bv, wo):
    rows, width = x.shape
    slots, dim = kc.shape[1], kc.shape[3]
    flat = rows * dim
    kt = jnp.transpose(kc, (0, 2, 3, 1)).reshape(flat, slots)
    vt = jnp.transpose(vc, (0, 2, 3, 1)).reshape(flat, slots)
    steps = rows // (SEQ * SUB)
    vmem = pl.BlockSpec(memory_space=pltpu.VMEM)
    hbm = pl.BlockSpec(memory_space=pltpu.HBM)
    dma = pltpu.SemaphoreType.DMA
    ko, vo, part = pl.pallas_call(
        attn_kernel,
        out_shape=(jax.ShapeDtypeStruct((flat, slots), BF16), jax.ShapeDtypeStruct((flat, slots), BF16),
                   jax.ShapeDtypeStruct((rows, width), BF16)),
        in_specs=[hbm] * 12,
        out_specs=(hbm, hbm, hbm),
        scratch_shapes=[pltpu.VMEM((flat, slots), BF16), pltpu.VMEM((flat, slots), BF16),
                        pltpu.VMEM(wq.shape, BF16), pltpu.VMEM((2 * dim, width), BF16), pltpu.VMEM(wo.shape, BF16),
                        pltpu.VMEM((rows, rows), F32), pltpu.VMEM((4, rows, 2 * dim), F32),
                        pltpu.VMEM((2 * dim, rows), BF16), pltpu.VMEM((rows, 4 * dim), F32),
                        pltpu.VMEM(x.shape, BF16), pltpu.SMEM((rows,), jnp.int32), pltpu.VMEM((rows,), jnp.int32), pltpu.VMEM(x.shape, BF16),
                        pltpu.VMEM(g.shape, BF16), pltpu.VMEM(bq.shape, BF16), pltpu.VMEM(bk.shape, BF16),
                        pltpu.VMEM(bv.shape, BF16),
                        dma((steps,)), dma((steps,)), dma((steps,)), dma((steps,)), dma((5,)), dma((7,))],
        compiler_params=pltpu.CompilerParams(vmem_limit_bytes=VMEM_ALL),
        name='attn',
    )(lens, x, g, bq, bk, bv, kt, vt, wq, wk.T, wv.T, wo)
    back = lambda c: jnp.transpose(c.reshape(rows, 1, dim, slots), (0, 3, 1, 2))
    return part, back(ko), back(vo)


CHUNK = 512
SLOTS = 26
MLP_SLOTS = 6
EARLY = 10
BLOCK = 256
CHEW = ((0, 5, 5), (0, 5, 5))
LOW = -1e30
GROUP = 3


def tail_kernel(part, x, tok, gm, gf, wg, wu, wd, wh,
                y_s, stats,
                buf, last_v, d2d, xs, xr, m_s, a_s, h_s, p_s, f_s, acc, acd, tok_c, tok_r, st_s, st_r,
                part_ref, x_v, tok_v, gm_v, gf_v,
                w_sem, h_sem, d_send, d_recv, x_send, x_recv, g_send, g_recv, f_send, f_recv, s_send, s_recv):
    me = lax.axis_index('tp')
    n_tp = 2 * xs.shape[1]
    chips = n_tp // 2
    xi, core = me // 2, me % 2
    sibling = {'tp': me + 1 - 2 * core}
    rows, width = part.shape
    half = rows // 2
    piece = half // chips
    ff = wg.shape[1]
    vocab = wh.shape[0]
    full = vocab // CHUNK
    rest = vocab - full * CHUNK

    def rows_of(side, chip):
        return pl.ds(pl.multiple_of(side * half + chip * piece, piece), piece)

    mine = rows_of(core, xi)

    small = [pltpu.make_async_copy(x.at[mine], x_v, w_sem.at[0]), pltpu.make_async_copy(tok, tok_v, w_sem.at[1]),
             pltpu.make_async_copy(gm, gm_v, w_sem.at[2]), pltpu.make_async_copy(gf, gf_v, w_sem.at[3]),
             pltpu.make_async_copy(part, part_ref, w_sem.at[15])]
    last_copy = pltpu.make_async_copy(wh.at[pl.ds(full * CHUNK, rest)], last_v, w_sem.at[4])
    mlp_copies = []
    for n, w in enumerate((wg, wu)):
        for kb in range(width // CHUNK):
            mlp_copies.append(pltpu.make_async_copy(
                w.at[pl.ds(kb * CHUNK, CHUNK)], buf.at[2 * n + kb // 2, :, pl.ds((kb % 2) * ff, ff)],
                w_sem.at[5 + 4 * n + kb]))
    for kb in range(ff // CHUNK):
        mlp_copies.append(pltpu.make_async_copy(wd.at[pl.ds(kb * CHUNK, CHUNK)], buf.at[4 + kb], w_sem.at[13 + kb]))

    def slot_of(i):
        return lax.rem(i + MLP_SLOTS, SLOTS)

    def head_copy(i):
        return pltpu.make_async_copy(wh.at[pl.ds(pl.multiple_of(i * CHUNK, CHUNK), CHUNK)], buf.at[slot_of(i)],
                                     h_sem.at[slot_of(i)])

    def head_begin(i, carry):
        head_copy(i).start()
        return carry

    for copy in small:
        copy.start()
    lax.fori_loop(0, EARLY, head_begin, 0)
    for copy in mlp_copies:
        copy.start()
    lax.fori_loop(EARLY, SLOTS - MLP_SLOTS, head_begin, 0)
    last_copy.start()

    barrier = pltpu.get_barrier_semaphore()
    for k in range(1, n_tp):
        pl.semaphore_signal(barrier, inc=1, device_id={'tp': lax.rem(me + k, n_tp)}, device_id_type=MESH)

    acd[0] = jnp.full((8, rows), LOW, F32)
    acd[1] = jnp.zeros((8, rows), F32)
    acd[2] = jnp.zeros((8, rows), F32)
    acc[0] = jnp.full((rows, 128), LOW, F32)
    acc[1] = jnp.zeros((rows, 128), F32)
    acc[2] = jnp.zeros((rows, 128), F32)
    for copy in small:
        copy.wait()
    tok_row = (tok_v[...].reshape(1, rows) - me * vocab).astype(F32)
    tok_row = jnp.where((tok_row >= 0) & (tok_row < vocab), tok_row, -float(2 * vocab))
    tok_r[...] = jnp.broadcast_to(tok_row, (8, rows)).astype(jnp.int32)
    tok_c[...] = jnp.transpose(jnp.broadcast_to(tok_row, (rows, rows))).astype(jnp.int32)

    pl.semaphore_wait(barrier, n_tp - 1)

    turned = [0]

    def chew(count):
        first = turned[0]
        turned[0] += count

        def one(i, carry):
            head_copy(i).wait()
            slot = slot_of(i)

            def strip(c, inner):
                cols = pl.ds(pl.multiple_of(c * CHUNK, CHUNK), CHUNK)
                buf[slot, :, cols] = jnp.transpose(buf[slot, :, cols])
                return inner

            lax.fori_loop(0, width // CHUNK, strip, 0)
            return carry

        if count:
            lax.fori_loop(first, first + count, one, 0)

    def exchange(rnd, src, full_ref, finish):
        order = [2, 1, 3]

        def pair_copy(k):
            chip = lax.rem(xi + k, chips)
            return pltpu.make_async_remote_copy(
                src_ref=src.at[rows_of(1 - core, chip)], dst_ref=d2d.at[rnd, k],
                send_sem=d_send.at[rnd, k], recv_sem=d_recv.at[rnd, k], device_id=sibling, device_id_type=MESH)

        def ring_copy(k):
            return pltpu.make_async_remote_copy(
                src_ref=xs.at[rnd, k], dst_ref=xr.at[rnd, k], send_sem=x_send.at[rnd, k], recv_sem=x_recv.at[rnd, k],
                device_id={'tp': lax.rem(xi + k, chips) * 2 + core}, device_id_type=MESH)

        def share_copy(k):
            return pltpu.make_async_remote_copy(
                src_ref=full_ref.at[mine], dst_ref=full_ref.at[mine], send_sem=g_send.at[rnd, k], recv_sem=g_recv.at[rnd, k],
                device_id={'tp': lax.rem(xi + k, chips) * 2 + core}, device_id_type=MESH)

        def forward_copy(k):
            its = rows_of(core, lax.rem(xi + chips - k, chips))
            return pltpu.make_async_remote_copy(
                src_ref=full_ref.at[its], dst_ref=full_ref.at[its], send_sem=f_send.at[rnd, k], recv_sem=f_recv.at[rnd, k],
                device_id=sibling, device_id_type=MESH)

        for k in order + [0]:
            pair_copy(k).start()
        chew(CHEW[rnd][0])
        for k in order:
            pair_copy(k).wait_recv()
            chip = lax.rem(xi + k, chips)
            xs[rnd, k] = (src[rows_of(core, chip), :].astype(F32) + d2d[rnd, k].astype(F32)).astype(BF16)
            ring_copy(k).start()
        pair_copy(0).wait_recv()
        chew(CHEW[rnd][1])
        total = src[mine, :].astype(F32) + d2d[rnd, 0].astype(F32)
        for k in (1, 3, 2):
            ring_copy(k).wait_recv()
            total = total + xr[rnd, k].astype(F32)
        full_ref[mine, :] = finish(total)
        for k in order:
            share_copy(k).start()
        forward_copy(0).start()
        chew(CHEW[rnd][2])
        for k in (1, 3, 2):
            share_copy(k).wait_recv()
            forward_copy(k).start()
        for k in range(chips):
            forward_copy(k).wait_recv()
        for k in range(chips):
            pair_copy(k).wait_send()
            forward_copy(k).wait_send()
            if k:
                ring_copy(k).wait_send()
                share_copy(k).wait_send()

    def finish_attn(total):
        a = (x_v[...].astype(F32) + total).astype(BF16)
        a_s[...] = a
        return rms(a.astype(F32), gm_v[...].astype(F32).reshape(1, -1))

    exchange(0, part_ref, m_s, finish_attn)

    for copy in mlp_copies:
        copy.wait()

    def gate_up(j, carry):
        def product(n):
            out = None
            for kb in range(width // CHUNK):
                cols = pl.ds(pl.multiple_of((kb % 2) * ff + j * BLOCK, BLOCK), BLOCK)
                term = jnp.dot(m_s[:, kb * CHUNK:(kb + 1) * CHUNK], buf[2 * n + kb // 2, :, cols], preferred_element_type=F32)
                out = term if out is None else out + term
            return out

        gate = product(0)
        up = product(1)
        h_s[:, pl.ds(pl.multiple_of(j * BLOCK, BLOCK), BLOCK)] = (gate * jax.nn.sigmoid(gate) * up).astype(BF16)
        return carry

    lax.fori_loop(0, ff // BLOCK, gate_up, 0)

    def down(j, carry):
        cols = pl.ds(pl.multiple_of(j * CHUNK, CHUNK), CHUNK)
        out = jnp.dot(h_s[:, :CHUNK], buf[4, :, cols], preferred_element_type=F32)
        out = out + jnp.dot(h_s[:, CHUNK:], buf[5, :, cols], preferred_element_type=F32)
        p_s[:, cols] = out.astype(BF16)
        return carry

    lax.fori_loop(0, width // CHUNK, down, 0)
    lax.fori_loop(SLOTS - MLP_SLOTS, SLOTS, head_begin, 0)

    exchange(1, p_s, y_s, lambda total: (a_s[...].astype(F32) + total).astype(BF16))

    f_s[...] = rms(y_s[...].astype(F32), gf_v[...].astype(F32).reshape(1, -1))

    lane = lax.broadcasted_iota(jnp.int32, (rows, 128), 1)

    def fold_across(scores, first_row):
        parts = [scores[:, j * 128:(j + 1) * 128] for j in range(scores.shape[1] // 128)]
        old = acc[0]
        top = functools.reduce(jnp.maximum, parts, old)
        total = acc[1] * jnp.exp(old - top)
        target = acc[2]
        place = tok_c[...] - first_row
        for j, part in enumerate(parts):
            total = total + jnp.exp(part - top)
            target = target + jnp.where(place == lane + j * 128, part, 0.0)
        acc[0] = top
        acc[1] = total
        acc[2] = target

    def fold_down(scores, first_row):
        groups = scores.reshape(scores.shape[0] // 8, 8, rows)
        old = acd[0]
        top = jnp.maximum(old, jnp.max(groups, axis=0))
        acd[1] = acd[1] * jnp.exp(old - top) + jnp.sum(jnp.exp(groups - top[None]), axis=0)
        ids = lax.broadcasted_iota(jnp.int32, scores.shape, 0)
        hit = ids == (tok_r[0:1, :] - first_row)
        acd[2] = acd[2] + jnp.sum(jnp.where(hit, scores, 0.0).reshape(groups.shape), axis=0)
        acd[0] = top

    def turned_chunk(i):
        slot = slot_of(i)
        scores = []
        for r in range(CHUNK // BLOCK):
            out = None
            for c in range(width // CHUNK):
                for n in range(CHUNK // BLOCK):
                    term = jnp.dot(f_s[:, c * CHUNK + n * BLOCK:c * CHUNK + (n + 1) * BLOCK],
                                   buf[slot, n * BLOCK:(n + 1) * BLOCK, c * CHUNK + r * BLOCK:c * CHUNK + (r + 1) * BLOCK],
                                   preferred_element_type=F32)
                    out = term if out is None else out + term
            scores.append(out)
        fold_across(jnp.concatenate(scores, axis=1), i * CHUNK)

    def plain_chunk(i):
        scores = lax.dot_general(buf[slot_of(i)], f_s[...], NT, preferred_element_type=F32)
        fold_down(scores, i * CHUNK)

    def refill(i):
        @pl.when(i + SLOTS < full)
        def _():
            head_copy(i + SLOTS).start()

    def sweep(first, count, size, take, fresh):
        def run(n, carry):
            at = [first + n * size + u for u in range(size)]
            if fresh:
                for i in at:
                    head_copy(i).wait()
            for i in at:
                take(i)
            for i in at:
                refill(i)
            return carry

        if count >= size:
            lax.fori_loop(0, count // size, run, 0)
        if count % size:
            sweep(first + count // size * size, count % size, count % size, take, fresh)

    sweep(0, turned[0], GROUP, turned_chunk, False)
    sweep(turned[0], full - turned[0], GROUP, plain_chunk, True)
    last_copy.wait()
    fold_down(lax.dot_general(last_v[...], f_s[...], NT, preferred_element_type=F32), full * CHUNK)

    tops = jnp.transpose(acc[0])
    top = jnp.maximum(jnp.max(tops, axis=0, keepdims=True), jnp.max(acd[0], axis=0, keepdims=True))
    total = (jnp.sum(jnp.transpose(acc[1]) * jnp.exp(tops - top), axis=0, keepdims=True)
             + jnp.sum(acd[1] * jnp.exp(acd[0] - top), axis=0, keepdims=True))
    target = jnp.sum(jnp.transpose(acc[2]), axis=0, keepdims=True) + jnp.sum(acd[2], axis=0, keepdims=True)
    st_s[...] = jnp.concatenate([top, total, target, jnp.zeros((5, rows), F32)], axis=0)

    def stat_copy(k):
        return pltpu.make_async_remote_copy(
            src_ref=st_s, dst_ref=st_r.at[k], send_sem=s_send.at[k], recv_sem=s_recv.at[k],
            device_id={'tp': lax.rem(me + k, n_tp)}, device_id_type=MESH)

    for k in range(1, n_tp):
        stat_copy(k).start()
    for k in range(1, n_tp):
        stat_copy(k).wait_recv()
    tops = [top] + [st_r[k, 0:1, :] for k in range(1, n_tp)]
    totals = [total] + [st_r[k, 1:2, :] for k in range(1, n_tp)]
    best = functools.reduce(jnp.maximum, tops)
    mass = sum(s * jnp.exp(t - best) for s, t in zip(totals, tops))
    hit = target + sum(st_r[k, 2:3, :] for k in range(1, n_tp))
    lse = best + jnp.log(mass)
    stats[...] = jnp.concatenate([hit - lse, lse, jnp.zeros((6, rows), F32)], axis=0)
    for k in range(1, n_tp):
        stat_copy(k).wait_send()


def tail(part, x, tok, gm, gf, wg, wu, wd, wh, n_tp):
    rows, width = x.shape
    chips = n_tp // 2
    piece = rows // n_tp
    vmem = pl.BlockSpec(memory_space=pltpu.VMEM)
    hbm = pl.BlockSpec(memory_space=pltpu.HBM)
    dma = pltpu.SemaphoreType.DMA
    rest = wh.shape[0] % CHUNK
    return pl.pallas_call(
        tail_kernel,
        out_shape=(jax.ShapeDtypeStruct((rows, width), BF16), jax.ShapeDtypeStruct((8, rows), F32)),
        in_specs=[hbm] * 9,
        out_specs=(vmem, vmem),
        scratch_shapes=[pltpu.VMEM((SLOTS, CHUNK, width), BF16), pltpu.VMEM((rest, width), BF16),
                        pltpu.VMEM((2, chips, piece, width), BF16), pltpu.VMEM((2, chips, piece, width), BF16),
                        pltpu.VMEM((2, chips, piece, width), BF16),
                        pltpu.VMEM((rows, width), BF16), pltpu.VMEM((piece, width), BF16),
                        pltpu.VMEM((rows, wg.shape[1]), BF16),
                        pltpu.VMEM((rows, width), BF16), pltpu.VMEM((rows, width), BF16),
                        pltpu.VMEM((3, rows, 128), F32), pltpu.VMEM((3, 8, rows), F32),
                        pltpu.VMEM((rows, rows), jnp.int32), pltpu.VMEM((8, rows), jnp.int32),
                        pltpu.VMEM((8, rows), F32), pltpu.VMEM((n_tp, 8, rows), F32),
                        pltpu.VMEM((rows, width), BF16), pltpu.VMEM((piece, width), BF16), pltpu.VMEM((rows,), jnp.int32),
                        pltpu.VMEM(gm.shape, BF16), pltpu.VMEM(gf.shape, BF16),
                        dma((16,)), dma((SLOTS,)),
                        dma((2, chips)), dma((2, chips)), dma((2, chips)), dma((2, chips)),
                        dma((2, chips)), dma((2, chips)), dma((2, chips)), dma((2, chips)),
                        dma((n_tp,)), dma((n_tp,))],
        compiler_params=pltpu.CompilerParams(vmem_limit_bytes=VMEM_TAIL, collective_id=0, has_side_effects=True),
        name='tail',
    )(part, x, tok, gm, gf, wg, wu, wd, wh)


VMEM_TAIL = VMEM_ALL


def give_kernel(y, stats, y_out, logp_out, lse_out, sem):
    copy = pltpu.make_async_copy(y, y_out, sem)
    copy.start()
    logp_out[...] = stats[0:1, :].reshape(stats.shape[1])
    lse_out[...] = stats[1:2, :].reshape(stats.shape[1])
    copy.wait()


def give(y, stats):
    rows = y.shape[0]
    vmem = pl.BlockSpec(memory_space=pltpu.VMEM)
    return pl.pallas_call(
        give_kernel,
        out_shape=(jax.ShapeDtypeStruct(y.shape, BF16), jax.ShapeDtypeStruct((rows,), F32), jax.ShapeDtypeStruct((rows,), F32)),
        in_specs=[vmem, vmem],
        out_specs=(pl.BlockSpec(memory_space=pltpu.HBM), vmem, vmem),
        scratch_shapes=[pltpu.SemaphoreType.DMA],
        compiler_params=pltpu.CompilerParams(vmem_limit_bytes=VMEM_TAIL),
        name='give',
    )(y, stats)


def solution(mesh):
    n_tp = mesh.shape['tp']

    def local_step(tok_hidden, seq_lens, k_cache, v_cache, next_tok, g_attn, w_q, b_q, w_k, b_k, w_v, b_v, w_o, g_mlp,
                   w_gate, w_up, w_down, g_final, w_head):
        part, k_all, v_all = attention(tok_hidden, seq_lens, k_cache, v_cache, g_attn, w_q, b_q, w_k, b_k, w_v, b_v, w_o)
        y_all, stats = tail(part, tok_hidden, next_tok, g_mlp, g_final, w_gate, w_up, w_down, w_head, n_tp)
        y_out, tok_logp, norm_lse = give(y_all, stats)
        return y_out, k_all, v_all, tok_logp, norm_lse

    row_spec = P('dp', None)
    vec_spec = P('dp')
    cache_spec = P('dp', None, 'tp', None)
    col_spec = P(None, 'tp')
    part_spec = P('tp')
    whole_spec = P(None)
    in_specs = (row_spec, vec_spec, cache_spec, cache_spec, vec_spec, whole_spec, col_spec, part_spec, col_spec, part_spec,
                col_spec, part_spec, P('tp', None), whole_spec, col_spec, col_spec, P('tp', None), whole_spec, P('tp', None))
    out_specs = (row_spec, cache_spec, cache_spec, vec_spec, vec_spec)
    return jax.shard_map(local_step, mesh=mesh, in_specs=in_specs, out_specs=out_specs, check_vma=False)
```

```python
import functools
import math
import jax
import jax.numpy as jnp
from jax import lax
from jax.experimental import pallas as pl
from jax.experimental.pallas import tpu as pltpu
from jax.sharding import PartitionSpec as P

THETA = 1000000.0
EPS = 1e-6
MESH = pl.DeviceIdType.MESH
NT = (((1,), (1,)), ((), ()))
F32 = jnp.float32
BF16 = jnp.bfloat16


def rms(vals_f32, gain_f32):
    inv_rms = lax.rsqrt(jnp.mean(vals_f32 * vals_f32, axis=-1, keepdims=True) + EPS)
    return (vals_f32 * inv_rms * gain_f32).astype(BF16)


VMEM_ALL = 67043328
SEQ = 8
SUB = 2


def attn_kernel(lens, x, g, bq, bk, bv, kc, vc, wq, wk, wv,
                ko, vo, heads, kbuf, vbuf, wq_v, wkv_v, lens_b, qq, kvt, o_s,
                heads_s, lens_s, lens_v, x_ref, g_ref, bq_ref, bk_ref, bv_ref,
                k_in, v_in, k_out, v_out, w_sem, i_sem):
    rows = x_ref.shape[0]
    dim = wk.shape[0]
    slots = kbuf.shape[1]
    span = SEQ * SUB * dim
    steps = kbuf.shape[0] // span

    small = [pltpu.make_async_copy(src, dst, i_sem.at[n]) for n, (src, dst) in enumerate(
        [(x, x_ref), (g, g_ref), (lens, lens_v), (lens, lens_s), (bq, bq_ref), (bk, bk_ref), (bv, bv_ref)])]
    for copy in small:
        copy.start()
    w_copies = [pltpu.make_async_copy(wq, wq_v, w_sem.at[0]),
                pltpu.make_async_copy(wk, wkv_v.at[pl.ds(0, dim)], w_sem.at[1]),
                pltpu.make_async_copy(wv, wkv_v.at[pl.ds(dim, dim)], w_sem.at[2])]
    for copy in w_copies:
        copy.start()

    def moves(step):
        here = pl.ds(pl.multiple_of(step * span, span), span)
        return (pltpu.make_async_copy(kc.at[here], kbuf.at[here], k_in.at[step]),
                pltpu.make_async_copy(vc.at[here], vbuf.at[here], v_in.at[step]),
                pltpu.make_async_copy(kbuf.at[here], ko.at[here], k_out.at[step]),
                pltpu.make_async_copy(vbuf.at[here], vo.at[here], v_out.at[step]))

    def begin(step, carry):
        k_copy, v_copy, _, _ = moves(step)
        k_copy.start()
        v_copy.start()
        return carry

    lax.fori_loop(0, steps, begin, 0)

    for copy in small:
        copy.wait()
    normed = rms(x_ref[...].astype(F32), g_ref[...].astype(F32).reshape(1, -1))
    lens_row = lens_v[...].reshape(1, rows).astype(F32)
    lens_col = jnp.transpose(jnp.broadcast_to(lens_row, (rows, rows)))
    lens_b[...] = lens_col
    lane = lax.broadcasted_iota(jnp.int32, (rows, 2 * dim), 1)
    low = lane < dim
    first = (lane & (dim - 1)) < dim // 2
    power = (lane & (dim // 2 - 1)).astype(F32) * (-2.0 / dim)
    angles = lens_col * jnp.exp(power * math.log(THETA))
    cos_t = jnp.cos(angles)
    sin_t = jnp.where(first, -jnp.sin(angles), jnp.sin(angles))

    def rope(vals):
        partner = jnp.where(first, pltpu.roll(vals, 2 * dim - dim // 2, 1), pltpu.roll(vals, dim // 2, 1))
        return vals * cos_t + partner * sin_t

    w_copies[1].wait()
    w_copies[2].wait()
    kv = lax.dot_general(normed, wkv_v[...], NT, preferred_element_type=F32)
    bkv = jnp.concatenate([bk_ref[...].astype(F32).reshape(1, dim), bv_ref[...].astype(F32).reshape(1, dim)], axis=1)
    kv = kv + bkv
    kv = jnp.where(low, rope(kv), kv).astype(BF16).astype(F32)
    kvt[...] = jnp.transpose(kv).astype(BF16)
    w_copies[0].wait()
    q_all = jnp.dot(normed, wq_v[...], preferred_element_type=F32) + bq_ref[...].astype(F32).reshape(1, -1)
    for half in range(2):
        q_half = rope(q_all[:, half * 2 * dim:(half + 1) * 2 * dim]).astype(BF16).astype(F32)
        swapped = pltpu.roll(q_half, dim, 1)
        qq[2 * half] = jnp.where(low, q_half, swapped)
        qq[2 * half + 1] = jnp.where(low, swapped, q_half)

    def body(step, carry):
        k_copy, v_copy, k_back, v_back = moves(step)
        base = pl.multiple_of(step * span, span)
        row0 = pl.multiple_of(step * (SEQ * SUB), SEQ * SUB)
        count = SEQ * SUB
        pick = (lax.broadcasted_iota(jnp.int32, (rows, count * 128), 0)
                == row0 + (lax.broadcasted_iota(jnp.int32, (rows, count * 128), 1) >> 7))
        fresh = jnp.dot(kvt[...], jnp.where(pick, 1.0, 0.0).astype(BF16), preferred_element_type=F32)
        k_copy.wait()
        v_copy.wait()
        lane_id = lax.broadcasted_iota(jnp.int32, (dim, 128), 1)
        for i in range(count):
            length = lens_s[row0 + i]
            start = pl.multiple_of((length >> 7) << 7, 128)
            hit = lane_id == (length - start)
            tile = fresh[:, i * 128:(i + 1) * 128]
            where_k = (pl.ds(base + i * dim, dim), pl.ds(start, 128))
            kbuf[where_k] = jnp.where(hit, tile[:dim], kbuf[where_k].astype(F32)).astype(BF16)
            vbuf[where_k] = jnp.where(hit, tile[dim:], vbuf[where_k].astype(F32)).astype(BF16)
        k_back.start()
        v_back.start()
        own = (lax.broadcasted_iota(jnp.int32, (SEQ, SEQ * dim), 1) // dim
               == lax.broadcasted_iota(jnp.int32, (SEQ, SEQ * dim), 0))
        slot = lax.broadcasted_iota(jnp.int32, (SEQ, slots), 1).astype(F32)
        scores = []
        for s in range(SUB):
            r0 = pl.multiple_of(row0 + s * SEQ, SEQ)
            q_blk = qq[:, pl.ds(r0, SEQ), :]
            wide = jnp.concatenate([q_blk] * (SEQ * dim // q_blk.shape[2]), axis=2)
            lhs = jnp.where(own[None], wide, 0.0).reshape(4 * SEQ, SEQ * dim).astype(BF16)
            keys = kbuf[pl.ds(base + s * SEQ * dim, SEQ * dim), :]
            scores.append(jnp.dot(lhs, keys, preferred_element_type=F32) * (dim ** -0.5))
        probs = []
        for s in range(SUB):
            r0 = pl.multiple_of(row0 + s * SEQ, SEQ)
            limit = lens_b[pl.ds(r0, SEQ), :][:, :1]
            masked = jnp.where((slot <= limit)[None], scores[s].reshape(4, SEQ, slots), -jnp.inf)
            top = jnp.max(masked, axis=-1, keepdims=True)
            weight = jnp.exp(masked - top)
            total = jnp.sum(weight, axis=-1, keepdims=True)
            probs.append((weight / total).reshape(4 * SEQ, slots).astype(BF16))
        for s in range(SUB):
            r0 = pl.multiple_of(row0 + s * SEQ, SEQ)
            vals = vbuf[pl.ds(base + s * SEQ * dim, SEQ * dim), :]
            out = lax.dot_general(probs[s], vals, NT, preferred_element_type=F32)
            out = jnp.where(own[None], out.reshape(4, SEQ, SEQ * dim), 0.0)
            width = 2 * dim
            fold = out[:, :, :width]
            for j in range(1, SEQ * dim // width):
                fold = fold + out[:, :, j * width:(j + 1) * width]
            fold = fold.reshape(4 * SEQ, width)
            fold = (fold + pltpu.roll(fold, dim, 1)).reshape(4, SEQ, width)
            low8 = lax.broadcasted_iota(jnp.int32, (SEQ, width), 1) < dim
            o_s[pl.ds(r0, SEQ), :width] = jnp.where(low8, fold[0], fold[1])
            o_s[pl.ds(r0, SEQ), width:] = jnp.where(low8, fold[2], fold[3])
        return carry

    lax.fori_loop(0, steps, body, 0)
    heads_s[...] = o_s[...].astype(BF16)
    heads_copy = pltpu.make_async_copy(heads_s, heads, w_sem.at[3])
    heads_copy.start()

    def finish(step, carry):
        _, _, k_back, v_back = moves(step)
        k_back.wait()
        v_back.wait()
        return carry

    lax.fori_loop(0, steps, finish, 0)
    heads_copy.wait()


def attention(x, lens, kc, vc, g, wq, bq, wk, bk, wv, bv):
    rows, width = x.shape
    slots, dim = kc.shape[1], kc.shape[3]
    flat = rows * dim
    kt = jnp.transpose(kc, (0, 2, 3, 1)).reshape(flat, slots)
    vt = jnp.transpose(vc, (0, 2, 3, 1)).reshape(flat, slots)
    steps = rows // (SEQ * SUB)
    vmem = pl.BlockSpec(memory_space=pltpu.VMEM)
    hbm = pl.BlockSpec(memory_space=pltpu.HBM)
    dma = pltpu.SemaphoreType.DMA
    ko, vo, heads = pl.pallas_call(
        attn_kernel,
        out_shape=(jax.ShapeDtypeStruct((flat, slots), BF16), jax.ShapeDtypeStruct((flat, slots), BF16),
                   jax.ShapeDtypeStruct((rows, 4 * dim), BF16)),
        in_specs=[hbm] * 11,
        out_specs=(hbm, hbm, hbm),
        scratch_shapes=[pltpu.VMEM((flat, slots), BF16), pltpu.VMEM((flat, slots), BF16),
                        pltpu.VMEM(wq.shape, BF16), pltpu.VMEM((2 * dim, width), BF16),
                        pltpu.VMEM((rows, rows), F32), pltpu.VMEM((4, rows, 2 * dim), F32),
                        pltpu.VMEM((2 * dim, rows), BF16), pltpu.VMEM((rows, 4 * dim), F32),
                        pltpu.VMEM((rows, 4 * dim), BF16), pltpu.SMEM((rows,), jnp.int32), pltpu.VMEM((rows,), jnp.int32), pltpu.VMEM(x.shape, BF16),
                        pltpu.VMEM(g.shape, BF16), pltpu.VMEM(bq.shape, BF16), pltpu.VMEM(bk.shape, BF16),
                        pltpu.VMEM(bv.shape, BF16),
                        dma((steps,)), dma((steps,)), dma((steps,)), dma((steps,)), dma((4,)), dma((7,))],
        compiler_params=pltpu.CompilerParams(vmem_limit_bytes=VMEM_ALL),
        name='attn',
    )(lens, x, g, bq, bk, bv, kt, vt, wq, wk.T, wv.T)
    back = lambda c: jnp.transpose(c.reshape(rows, 1, dim, slots), (0, 3, 1, 2))
    return heads, back(ko), back(vo)


CHUNK = 512
SLOTS = 26
MLP_SLOTS = 6
EARLY = 10
BLOCK = 256
CHEW = ((0, 5, 5), (0, 5, 5))
LOW = -1e30
GROUP = 4


def tail_kernel(heads, x, tok, gm, gf, wo, wg, wu, wd, wh,
                y_out, stats,
                buf, y_s, last_v, d2d, xs, xr, m_s, a_s, h_s, p_s, f_s, o_s, acc, acd, tok_c, tok_r, st_s, st_r,
                heads_v, x_v, tok_v, gm_v, gf_v,
                w_sem, h_sem, d_send, d_recv, x_send, x_recv, g_send, g_recv, f_send, f_recv, s_send, s_recv):
    me = lax.axis_index('tp')
    n_tp = 2 * xs.shape[1]
    chips = n_tp // 2
    xi, core = me // 2, me % 2
    sibling = {'tp': me + 1 - 2 * core}
    rows, width = p_s.shape
    half = rows // 2
    piece = half // chips
    ff = wg.shape[1]
    vocab = wh.shape[0]
    full = vocab // CHUNK
    rest = vocab - full * CHUNK

    def rows_of(side, chip):
        return pl.ds(pl.multiple_of(side * half + chip * piece, piece), piece)

    mine = rows_of(core, xi)

    small = [pltpu.make_async_copy(x.at[mine], x_v, w_sem.at[0]), pltpu.make_async_copy(tok, tok_v, w_sem.at[1]),
             pltpu.make_async_copy(gm, gm_v, w_sem.at[2]), pltpu.make_async_copy(gf, gf_v, w_sem.at[3]),
             pltpu.make_async_copy(heads, heads_v, w_sem.at[15]),
             pltpu.make_async_copy(wo, buf.at[SLOTS - 1, pl.ds(0, wo.shape[0])], w_sem.at[16])]
    last_copy = pltpu.make_async_copy(wh.at[pl.ds(full * CHUNK, rest)], last_v, w_sem.at[4])
    mlp_copies = []
    for n, w in enumerate((wg, wu)):
        for kb in range(width // CHUNK):
            mlp_copies.append(pltpu.make_async_copy(
                w.at[pl.ds(kb * CHUNK, CHUNK)], buf.at[2 * n + kb // 2, :, pl.ds((kb % 2) * ff, ff)],
                w_sem.at[5 + 4 * n + kb]))
    for kb in range(ff // CHUNK):
        mlp_copies.append(pltpu.make_async_copy(wd.at[pl.ds(kb * CHUNK, CHUNK)], buf.at[4 + kb], w_sem.at[13 + kb]))

    def slot_of(i):
        return lax.rem(i + MLP_SLOTS, SLOTS)

    def head_copy(i):
        return pltpu.make_async_copy(wh.at[pl.ds(pl.multiple_of(i * CHUNK, CHUNK), CHUNK)], buf.at[slot_of(i)],
                                     h_sem.at[slot_of(i)])

    def head_begin(i, carry):
        head_copy(i).start()
        return carry

    for copy in small:
        copy.start()
    lax.fori_loop(0, EARLY, head_begin, 0)
    for copy in mlp_copies:
        copy.start()
    lax.fori_loop(EARLY, SLOTS - MLP_SLOTS - 1, head_begin, 0)
    last_copy.start()

    barrier = pltpu.get_barrier_semaphore()
    for k in range(1, n_tp):
        pl.semaphore_signal(barrier, inc=1, device_id={'tp': lax.rem(me + k, n_tp)}, device_id_type=MESH)

    acd[0] = jnp.full((8, rows), LOW, F32)
    acd[1] = jnp.zeros((8, rows), F32)
    acd[2] = jnp.zeros((8, rows), F32)
    acc[0] = jnp.full((rows, 128), LOW, F32)
    acc[1] = jnp.zeros((rows, 128), F32)
    acc[2] = jnp.zeros((rows, 128), F32)
    for copy in small:
        copy.wait()
    tok_row = (tok_v[...].reshape(1, rows) - me * vocab).astype(F32)
    tok_row = jnp.where((tok_row >= 0) & (tok_row < vocab), tok_row, -float(2 * vocab))
    tok_r[...] = jnp.broadcast_to(tok_row, (8, rows)).astype(jnp.int32)
    tok_c[...] = jnp.transpose(jnp.broadcast_to(tok_row, (rows, rows))).astype(jnp.int32)

    o_s[...] = jnp.dot(heads_v[...], buf[SLOTS - 1, :wo.shape[0], :], preferred_element_type=F32).astype(BF16)
    head_copy(SLOTS - MLP_SLOTS - 1).start()
    pl.semaphore_wait(barrier, n_tp - 1)

    turned = [0]

    def chew(count):
        first = turned[0]
        turned[0] += count

        def one(i, carry):
            head_copy(i).wait()
            slot = slot_of(i)

            def strip(c, inner):
                cols = pl.ds(pl.multiple_of(c * CHUNK, CHUNK), CHUNK)
                buf[slot, :, cols] = jnp.transpose(buf[slot, :, cols])
                return inner

            lax.fori_loop(0, width // CHUNK, strip, 0)
            return carry

        if count:
            lax.fori_loop(first, first + count, one, 0)

    def exchange(rnd, src, full_ref, finish, landed):
        order = [2, 1, 3]

        def pair_copy(k):
            chip = lax.rem(xi + k, chips)
            return pltpu.make_async_remote_copy(
                src_ref=src.at[rows_of(1 - core, chip)], dst_ref=d2d.at[rnd, k],
                send_sem=d_send.at[rnd, k], recv_sem=d_recv.at[rnd, k], device_id=sibling, device_id_type=MESH)

        def ring_copy(k):
            return pltpu.make_async_remote_copy(
                src_ref=xs.at[rnd, k], dst_ref=xr.at[rnd, k], send_sem=x_send.at[rnd, k], recv_sem=x_recv.at[rnd, k],
                device_id={'tp': lax.rem(xi + k, chips) * 2 + core}, device_id_type=MESH)

        def share_copy(k):
            return pltpu.make_async_remote_copy(
                src_ref=full_ref.at[mine], dst_ref=full_ref.at[mine], send_sem=g_send.at[rnd, k], recv_sem=g_recv.at[rnd, k],
                device_id={'tp': lax.rem(xi + k, chips) * 2 + core}, device_id_type=MESH)

        def forward_copy(k):
            its = rows_of(core, lax.rem(xi + chips - k, chips))
            return pltpu.make_async_remote_copy(
                src_ref=full_ref.at[its], dst_ref=full_ref.at[its], send_sem=f_send.at[rnd, k], recv_sem=f_recv.at[rnd, k],
                device_id=sibling, device_id_type=MESH)

        for k in order + [0]:
            pair_copy(k).start()
        chew(CHEW[rnd][0])
        for k in order:
            pair_copy(k).wait_recv()
            chip = lax.rem(xi + k, chips)
            xs[rnd, k] = (src[rows_of(core, chip), :].astype(F32) + d2d[rnd, k].astype(F32)).astype(BF16)
            ring_copy(k).start()
        pair_copy(0).wait_recv()
        chew(CHEW[rnd][1])
        total = src[mine, :].astype(F32) + d2d[rnd, 0].astype(F32)
        for k in (1, 3, 2):
            ring_copy(k).wait_recv()
            total = total + xr[rnd, k].astype(F32)
        full_ref[mine, :] = finish(total)
        for k in order:
            share_copy(k).start()
        forward_copy(0).start()
        chew(CHEW[rnd][2])
        for k in (1, 3, 2):
            share_copy(k).wait_recv()
            forward_copy(k).start()
        landed(core)
        for k in range(chips):
            forward_copy(k).wait_recv()
        landed(1 - core)
        for k in range(chips):
            pair_copy(k).wait_send()
            forward_copy(k).wait_send()
            if k:
                ring_copy(k).wait_send()
                share_copy(k).wait_send()

    def finish_attn(total):
        a = (x_v[...].astype(F32) + total).astype(BF16)
        a_s[...] = a
        return rms(a.astype(F32), gm_v[...].astype(F32).reshape(1, -1))

    exchange(0, o_s, m_s, finish_attn, lambda side: None)

    for copy in mlp_copies:
        copy.wait()

    def widen(n):
        out = None
        for kb in range(width // CHUNK):
            term = jnp.dot(m_s[:, kb * CHUNK:(kb + 1) * CHUNK], buf[2 * n + kb // 2, :, (kb % 2) * ff:(kb % 2 + 1) * ff],
                           preferred_element_type=F32)
            out = term if out is None else out + term
        return out

    gate = widen(0)
    h_s[...] = (gate * jax.nn.sigmoid(gate) * widen(1)).astype(BF16)
    p_s[...] = (jnp.dot(h_s[:, :CHUNK], buf[4], preferred_element_type=F32)
                + jnp.dot(h_s[:, CHUNK:], buf[5], preferred_element_type=F32)).astype(BF16)
    lax.fori_loop(SLOTS - MLP_SLOTS, SLOTS, head_begin, 0)

    def final_norm(side):
        band = pl.ds(pl.multiple_of(side * half, half), half)
        f_s[band, :] = rms(y_s[band, :].astype(F32), gf_v[...].astype(F32).reshape(1, -1))

    exchange(1, p_s, y_s, lambda total: (a_s[...].astype(F32) + total).astype(BF16), final_norm)
    y_copy = pltpu.make_async_copy(y_s, y_out, w_sem.at[17])
    y_copy.start()

    lane = lax.broadcasted_iota(jnp.int32, (rows, 128), 1)

    def fold_across(scores, first_row):
        parts = [scores[:, j * 128:(j + 1) * 128] for j in range(scores.shape[1] // 128)]
        old = acc[0]
        top = functools.reduce(jnp.maximum, parts, old)
        total = acc[1] * jnp.exp(old - top)
        target = acc[2]
        place = tok_c[...] - first_row
        for j, part in enumerate(parts):
            total = total + jnp.exp(part - top)
            target = target + jnp.where(place == lane + j * 128, part, 0.0)
        acc[0] = top
        acc[1] = total
        acc[2] = target

    def fold_down(scores, first_row):
        groups = scores.reshape(scores.shape[0] // 8, 8, rows)
        old = acd[0]
        top = jnp.maximum(old, jnp.max(groups, axis=0))
        acd[1] = acd[1] * jnp.exp(old - top) + jnp.sum(jnp.exp(groups - top[None]), axis=0)
        ids = lax.broadcasted_iota(jnp.int32, scores.shape, 0)
        hit = ids == (tok_r[0:1, :] - first_row)
        acd[2] = acd[2] + jnp.sum(jnp.where(hit, scores, 0.0).reshape(groups.shape), axis=0)
        acd[0] = top

    def turned_chunk(i):
        slot = slot_of(i)
        scores = []
        for r in range(CHUNK // BLOCK):
            out = None
            for c in range(width // CHUNK):
                for n in range(CHUNK // BLOCK):
                    term = jnp.dot(f_s[:, c * CHUNK + n * BLOCK:c * CHUNK + (n + 1) * BLOCK],
                                   buf[slot, n * BLOCK:(n + 1) * BLOCK, c * CHUNK + r * BLOCK:c * CHUNK + (r + 1) * BLOCK],
                                   preferred_element_type=F32)
                    out = term if out is None else out + term
            scores.append(out)
        fold_across(jnp.concatenate(scores, axis=1), i * CHUNK)

    def plain_chunk(i):
        scores = lax.dot_general(buf[slot_of(i)], f_s[...], NT, preferred_element_type=F32)
        fold_down(scores, i * CHUNK)

    def refill(i):
        @pl.when(i + SLOTS < full)
        def _():
            head_copy(i + SLOTS).start()

    def sweep(first, count, size, take, fresh):
        def run(n, carry):
            at = [first + n * size + u for u in range(size)]
            if fresh:
                for i in at:
                    head_copy(i).wait()
            for i in at:
                take(i)
            for i in at:
                refill(i)
            return carry

        if count >= size:
            lax.fori_loop(0, count // size, run, 0)
        if count % size:
            sweep(first + count // size * size, count % size, count % size, take, fresh)

    sweep(0, turned[0], GROUP, turned_chunk, False)
    sweep(turned[0], full - turned[0], GROUP, plain_chunk, True)
    last_copy.wait()
    fold_down(lax.dot_general(last_v[...], f_s[...], NT, preferred_element_type=F32), full * CHUNK)

    tops = jnp.transpose(acc[0])
    top = jnp.maximum(jnp.max(tops, axis=0, keepdims=True), jnp.max(acd[0], axis=0, keepdims=True))
    total = (jnp.sum(jnp.transpose(acc[1]) * jnp.exp(tops - top), axis=0, keepdims=True)
             + jnp.sum(acd[1] * jnp.exp(acd[0] - top), axis=0, keepdims=True))
    target = jnp.sum(jnp.transpose(acc[2]), axis=0, keepdims=True) + jnp.sum(acd[2], axis=0, keepdims=True)
    st_s[...] = jnp.concatenate([top, total, target, jnp.zeros((5, rows), F32)], axis=0)

    def stat_copy(k):
        return pltpu.make_async_remote_copy(
            src_ref=st_s, dst_ref=st_r.at[k], send_sem=s_send.at[k], recv_sem=s_recv.at[k],
            device_id={'tp': lax.rem(me + k, n_tp)}, device_id_type=MESH)

    for k in range(1, n_tp):
        stat_copy(k).start()
    y_copy.wait()
    for k in range(1, n_tp):
        stat_copy(k).wait_recv()
    tops = [top] + [st_r[k, 0:1, :] for k in range(1, n_tp)]
    totals = [total] + [st_r[k, 1:2, :] for k in range(1, n_tp)]
    best = functools.reduce(jnp.maximum, tops)
    mass = sum(s * jnp.exp(t - best) for s, t in zip(totals, tops))
    hit = target + sum(st_r[k, 2:3, :] for k in range(1, n_tp))
    lse = best + jnp.log(mass)
    stats[...] = jnp.concatenate([hit - lse, lse, jnp.zeros((6, rows), F32)], axis=0)
    for k in range(1, n_tp):
        stat_copy(k).wait_send()


def tail(heads, x, tok, gm, gf, wo, wg, wu, wd, wh, n_tp):
    rows, width = x.shape
    chips = n_tp // 2
    piece = rows // n_tp
    vmem = pl.BlockSpec(memory_space=pltpu.VMEM)
    hbm = pl.BlockSpec(memory_space=pltpu.HBM)
    dma = pltpu.SemaphoreType.DMA
    rest = wh.shape[0] % CHUNK
    return pl.pallas_call(
        tail_kernel,
        out_shape=(jax.ShapeDtypeStruct((rows, width), BF16), jax.ShapeDtypeStruct((8, rows), F32)),
        in_specs=[hbm] * 10,
        out_specs=(hbm, vmem),
        scratch_shapes=[pltpu.VMEM((SLOTS, CHUNK, width), BF16), pltpu.VMEM((rows, width), BF16), pltpu.VMEM((rest, width), BF16),
                        pltpu.VMEM((2, chips, piece, width), BF16), pltpu.VMEM((2, chips, piece, width), BF16),
                        pltpu.VMEM((2, chips, piece, width), BF16),
                        pltpu.VMEM((rows, width), BF16), pltpu.VMEM((piece, width), BF16),
                        pltpu.VMEM((rows, wg.shape[1]), BF16),
                        pltpu.VMEM((rows, width), BF16), pltpu.VMEM((rows, width), BF16),
                        pltpu.VMEM((rows, width), BF16), pltpu.VMEM((3, rows, 128), F32), pltpu.VMEM((3, 8, rows), F32),
                        pltpu.VMEM((rows, rows), jnp.int32), pltpu.VMEM((8, rows), jnp.int32),
                        pltpu.VMEM((8, rows), F32), pltpu.VMEM((n_tp, 8, rows), F32),
                        pltpu.VMEM(heads.shape, BF16), pltpu.VMEM((piece, width), BF16), pltpu.VMEM((rows,), jnp.int32),
                        pltpu.VMEM(gm.shape, BF16), pltpu.VMEM(gf.shape, BF16),
                        dma((18,)), dma((SLOTS,)),
                        dma((2, chips)), dma((2, chips)), dma((2, chips)), dma((2, chips)),
                        dma((2, chips)), dma((2, chips)), dma((2, chips)), dma((2, chips)),
                        dma((n_tp,)), dma((n_tp,))],
        compiler_params=pltpu.CompilerParams(vmem_limit_bytes=VMEM_TAIL, collective_id=0, has_side_effects=True),
        name='tail',
    )(heads, x, tok, gm, gf, wo, wg, wu, wd, wh)


VMEM_TAIL = VMEM_ALL


PIECES = 4


def give_kernel(y, stats, y_out, logp_out, lse_out, y_v, s_v, in_sem, out_sem, s_sem):
    band = [pl.ds(n * (y.shape[0] // PIECES), y.shape[0] // PIECES) for n in range(PIECES)]
    reads = [pltpu.make_async_copy(y.at[b], y_v.at[b], in_sem.at[n]) for n, b in enumerate(band)]
    writes = [pltpu.make_async_copy(y_v.at[b], y_out.at[b], out_sem.at[n]) for n, b in enumerate(band)]
    stat_read = pltpu.make_async_copy(stats, s_v, s_sem)
    stat_read.start()
    for read in reads:
        read.start()
    stat_read.wait()
    logp_out[...] = s_v[0:1, :].reshape(s_v.shape[1])
    lse_out[...] = s_v[1:2, :].reshape(s_v.shape[1])
    for read, write in zip(reads, writes):
        read.wait()
        write.start()
    for write in writes:
        write.wait()


def give(y, stats):
    rows = y.shape[0]
    vmem = pl.BlockSpec(memory_space=pltpu.VMEM)
    hbm = pl.BlockSpec(memory_space=pltpu.HBM)
    dma = pltpu.SemaphoreType.DMA
    return pl.pallas_call(
        give_kernel,
        out_shape=(jax.ShapeDtypeStruct(y.shape, BF16), jax.ShapeDtypeStruct((rows,), F32), jax.ShapeDtypeStruct((rows,), F32)),
        in_specs=[hbm, hbm],
        out_specs=(hbm, vmem, vmem),
        scratch_shapes=[pltpu.VMEM(y.shape, BF16), pltpu.VMEM(stats.shape, F32), dma((PIECES,)), dma((PIECES,)), dma],
        compiler_params=pltpu.CompilerParams(vmem_limit_bytes=VMEM_ALL),
        name='give',
    )(y, stats)


def solution(mesh):
    n_tp = mesh.shape['tp']

    def local_step(tok_hidden, seq_lens, k_cache, v_cache, next_tok, g_attn, w_q, b_q, w_k, b_k, w_v, b_v, w_o, g_mlp,
                   w_gate, w_up, w_down, g_final, w_head):
        heads, k_all, v_all = attention(tok_hidden, seq_lens, k_cache, v_cache, g_attn, w_q, b_q, w_k, b_k, w_v, b_v)
        y_all, stats = tail(heads, tok_hidden, next_tok, g_mlp, g_final, w_o, w_gate, w_up, w_down, w_head, n_tp)
        y_out, tok_logp, norm_lse = give(y_all, stats)
        return y_out, k_all, v_all, tok_logp, norm_lse

    row_spec = P('dp', None)
    vec_spec = P('dp')
    cache_spec = P('dp', None, 'tp', None)
    col_spec = P(None, 'tp')
    part_spec = P('tp')
    whole_spec = P(None)
    in_specs = (row_spec, vec_spec, cache_spec, cache_spec, vec_spec, whole_spec, col_spec, part_spec, col_spec, part_spec,
                col_spec, part_spec, P('tp', None), whole_spec, col_spec, col_spec, P('tp', None), whole_spec, P('tp', None))
    out_specs = (row_spec, cache_spec, cache_spec, vec_spec, vec_spec)
    return jax.shard_map(local_step, mesh=mesh, in_specs=in_specs, out_specs=out_specs, check_vma=False)
```

```python
import functools
import math
import jax
import jax.numpy as jnp
from jax import lax
from jax.experimental import pallas as pl
from jax.experimental.pallas import tpu as pltpu
from jax.sharding import PartitionSpec as P

THETA = 1000000.0
EPS = 1e-6
MESH = pl.DeviceIdType.MESH
NT = (((1,), (1,)), ((), ()))
F32 = jnp.float32
BF16 = jnp.bfloat16


def rms(vals_f32, gain_f32):
    inv_rms = lax.rsqrt(jnp.mean(vals_f32 * vals_f32, axis=-1, keepdims=True) + EPS)
    return (vals_f32 * inv_rms * gain_f32).astype(BF16)


VMEM_ALL = 67043328
SEQ = 8
SUB = 2


def attn_kernel(lens, x, g, bq, bk, bv, kc, vc, wq, wk, wv,
                ko, vo, heads, kbuf, vbuf, wq_v, wkv_v, lens_b, qq, kvt, o_s,
                heads_s, lens_s, lens_v, x_ref, g_ref, bq_ref, bk_ref, bv_ref,
                k_in, v_in, k_out, v_out, w_sem, i_sem):
    rows = x_ref.shape[0]
    dim = wk.shape[0]
    slots = kbuf.shape[1]
    span = SEQ * SUB * dim
    steps = kbuf.shape[0] // span

    small = [pltpu.make_async_copy(src, dst, i_sem.at[n]) for n, (src, dst) in enumerate(
        [(x, x_ref), (g, g_ref), (lens, lens_v), (lens, lens_s), (bq, bq_ref), (bk, bk_ref), (bv, bv_ref)])]
    for copy in small:
        copy.start()
    w_copies = [pltpu.make_async_copy(wq, wq_v, w_sem.at[0]),
                pltpu.make_async_copy(wk, wkv_v.at[pl.ds(0, dim)], w_sem.at[1]),
                pltpu.make_async_copy(wv, wkv_v.at[pl.ds(dim, dim)], w_sem.at[2])]
    for copy in w_copies:
        copy.start()

    def moves(step):
        here = pl.ds(pl.multiple_of(step * span, span), span)
        return (pltpu.make_async_copy(kc.at[here], kbuf.at[here], k_in.at[step]),
                pltpu.make_async_copy(vc.at[here], vbuf.at[here], v_in.at[step]),
                pltpu.make_async_copy(kbuf.at[here], ko.at[here], k_out.at[step]),
                pltpu.make_async_copy(vbuf.at[here], vo.at[here], v_out.at[step]))

    def begin(step, carry):
        k_copy, v_copy, _, _ = moves(step)
        k_copy.start()
        v_copy.start()
        return carry

    lax.fori_loop(0, steps, begin, 0)

    for copy in small:
        copy.wait()
    normed = rms(x_ref[...].astype(F32), g_ref[...].astype(F32).reshape(1, -1))
    lens_row = lens_v[...].reshape(1, rows).astype(F32)
    lens_col = jnp.transpose(jnp.broadcast_to(lens_row, (rows, rows)))
    lens_b[...] = lens_col
    lane = lax.broadcasted_iota(jnp.int32, (rows, 2 * dim), 1)
    low = lane < dim
    first = (lane & (dim - 1)) < dim // 2
    power = (lane & (dim // 2 - 1)).astype(F32) * (-2.0 / dim)
    angles = lens_col * jnp.exp(power * math.log(THETA))
    cos_t = jnp.cos(angles)
    sin_t = jnp.where(first, -jnp.sin(angles), jnp.sin(angles))

    def rope(vals):
        partner = jnp.where(first, pltpu.roll(vals, 2 * dim - dim // 2, 1), pltpu.roll(vals, dim // 2, 1))
        return vals * cos_t + partner * sin_t

    w_copies[1].wait()
    w_copies[2].wait()
    kv = lax.dot_general(normed, wkv_v[...], NT, preferred_element_type=F32)
    bkv = jnp.concatenate([bk_ref[...].astype(F32).reshape(1, dim), bv_ref[...].astype(F32).reshape(1, dim)], axis=1)
    kv = kv + bkv
    kv = jnp.where(low, rope(kv), kv).astype(BF16).astype(F32)
    kvt[...] = jnp.transpose(kv).astype(BF16)
    w_copies[0].wait()
    q_all = jnp.dot(normed, wq_v[...], preferred_element_type=F32) + bq_ref[...].astype(F32).reshape(1, -1)
    for half in range(2):
        q_half = rope(q_all[:, half * 2 * dim:(half + 1) * 2 * dim]).astype(BF16).astype(F32)
        swapped = pltpu.roll(q_half, dim, 1)
        qq[2 * half] = jnp.where(low, q_half, swapped)
        qq[2 * half + 1] = jnp.where(low, swapped, q_half)

    def body(step, carry):
        k_copy, v_copy, k_back, v_back = moves(step)
        base = pl.multiple_of(step * span, span)
        row0 = pl.multiple_of(step * (SEQ * SUB), SEQ * SUB)
        count = SEQ * SUB
        pick = (lax.broadcasted_iota(jnp.int32, (rows, count * 128), 0)
                == row0 + (lax.broadcasted_iota(jnp.int32, (rows, count * 128), 1) >> 7))
        fresh = jnp.dot(kvt[...], jnp.where(pick, 1.0, 0.0).astype(BF16), preferred_element_type=F32)
        k_copy.wait()
        v_copy.wait()
        lane_id = lax.broadcasted_iota(jnp.int32, (dim, 128), 1)
        for i in range(count):
            length = lens_s[row0 + i]
            start = pl.multiple_of((length >> 7) << 7, 128)
            hit = lane_id == (length - start)
            tile = fresh[:, i * 128:(i + 1) * 128]
            where_k = (pl.ds(base + i * dim, dim), pl.ds(start, 128))
            kbuf[where_k] = jnp.where(hit, tile[:dim], kbuf[where_k].astype(F32)).astype(BF16)
            vbuf[where_k] = jnp.where(hit, tile[dim:], vbuf[where_k].astype(F32)).astype(BF16)
        k_back.start()
        v_back.start()
        own = (lax.broadcasted_iota(jnp.int32, (SEQ, SEQ * dim), 1) // dim
               == lax.broadcasted_iota(jnp.int32, (SEQ, SEQ * dim), 0))
        slot = lax.broadcasted_iota(jnp.int32, (SEQ, slots), 1).astype(F32)
        scores = []
        for s in range(SUB):
            r0 = pl.multiple_of(row0 + s * SEQ, SEQ)
            q_blk = qq[:, pl.ds(r0, SEQ), :]
            wide = jnp.concatenate([q_blk] * (SEQ * dim // q_blk.shape[2]), axis=2)
            lhs = jnp.where(own[None], wide, 0.0).reshape(4 * SEQ, SEQ * dim).astype(BF16)
            keys = kbuf[pl.ds(base + s * SEQ * dim, SEQ * dim), :]
            scores.append(jnp.dot(lhs, keys, preferred_element_type=F32) * (dim ** -0.5))
        probs = []
        for s in range(SUB):
            r0 = pl.multiple_of(row0 + s * SEQ, SEQ)
            limit = lens_b[pl.ds(r0, SEQ), :][:, :1]
            masked = jnp.where((slot <= limit)[None], scores[s].reshape(4, SEQ, slots), -jnp.inf)
            top = jnp.max(masked, axis=-1, keepdims=True)
            weight = jnp.exp(masked - top)
            total = jnp.sum(weight, axis=-1, keepdims=True)
            probs.append((weight / total).reshape(4 * SEQ, slots).astype(BF16))
        for s in range(SUB):
            r0 = pl.multiple_of(row0 + s * SEQ, SEQ)
            vals = vbuf[pl.ds(base + s * SEQ * dim, SEQ * dim), :]
            out = lax.dot_general(probs[s], vals, NT, preferred_element_type=F32)
            out = jnp.where(own[None], out.reshape(4, SEQ, SEQ * dim), 0.0)
            width = 2 * dim
            fold = out[:, :, :width]
            for j in range(1, SEQ * dim // width):
                fold = fold + out[:, :, j * width:(j + 1) * width]
            fold = fold.reshape(4 * SEQ, width)
            fold = (fold + pltpu.roll(fold, dim, 1)).reshape(4, SEQ, width)
            low8 = lax.broadcasted_iota(jnp.int32, (SEQ, width), 1) < dim
            o_s[pl.ds(r0, SEQ), :width] = jnp.where(low8, fold[0], fold[1])
            o_s[pl.ds(r0, SEQ), width:] = jnp.where(low8, fold[2], fold[3])
        return carry

    lax.fori_loop(0, steps, body, 0)
    heads_s[...] = o_s[...].astype(BF16)
    heads_copy = pltpu.make_async_copy(heads_s, heads, w_sem.at[3])
    heads_copy.start()

    def finish(step, carry):
        _, _, k_back, v_back = moves(step)
        k_back.wait()
        v_back.wait()
        return carry

    lax.fori_loop(0, steps, finish, 0)
    heads_copy.wait()


def attention(x, lens, kc, vc, g, wq, bq, wk, bk, wv, bv):
    rows, width = x.shape
    slots, dim = kc.shape[1], kc.shape[3]
    flat = rows * dim
    kt = jnp.transpose(kc, (0, 2, 3, 1)).reshape(flat, slots)
    vt = jnp.transpose(vc, (0, 2, 3, 1)).reshape(flat, slots)
    steps = rows // (SEQ * SUB)
    vmem = pl.BlockSpec(memory_space=pltpu.VMEM)
    hbm = pl.BlockSpec(memory_space=pltpu.HBM)
    dma = pltpu.SemaphoreType.DMA
    ko, vo, heads = pl.pallas_call(
        attn_kernel,
        out_shape=(jax.ShapeDtypeStruct((flat, slots), BF16), jax.ShapeDtypeStruct((flat, slots), BF16),
                   jax.ShapeDtypeStruct((rows, 4 * dim), BF16)),
        in_specs=[hbm] * 11,
        out_specs=(hbm, hbm, hbm),
        scratch_shapes=[pltpu.VMEM((flat, slots), BF16), pltpu.VMEM((flat, slots), BF16),
                        pltpu.VMEM(wq.shape, BF16), pltpu.VMEM((2 * dim, width), BF16),
                        pltpu.VMEM((rows, rows), F32), pltpu.VMEM((4, rows, 2 * dim), F32),
                        pltpu.VMEM((2 * dim, rows), BF16), pltpu.VMEM((rows, 4 * dim), F32),
                        pltpu.VMEM((rows, 4 * dim), BF16), pltpu.SMEM((rows,), jnp.int32), pltpu.VMEM((rows,), jnp.int32), pltpu.VMEM(x.shape, BF16),
                        pltpu.VMEM(g.shape, BF16), pltpu.VMEM(bq.shape, BF16), pltpu.VMEM(bk.shape, BF16),
                        pltpu.VMEM(bv.shape, BF16),
                        dma((steps,)), dma((steps,)), dma((steps,)), dma((steps,)), dma((4,)), dma((7,))],
        compiler_params=pltpu.CompilerParams(vmem_limit_bytes=VMEM_ALL),
        name='attn',
    )(lens, x, g, bq, bk, bv, kt, vt, wq, wk.T, wv.T)
    back = lambda c: jnp.transpose(c.reshape(rows, 1, dim, slots), (0, 3, 1, 2))
    return heads, back(ko), back(vo)


CHUNK = 512
SLOTS = 26
MLP_SLOTS = 6
EARLY = 10
BLOCK = 256
CHEW = ((0, 5, 5), (0, 5, 5))
LOW = -1e30
GROUP = 4


def tail_kernel(heads, x, tok, gm, gf, wo, wg, wu, wd, wh,
                y_out, stats,
                buf, y_s, last_v, d2d, xs, xr, m_s, a_s, h_s, p_s, f_s, o_s, acc, acd, tok_c, tok_r, st_s, st_r,
                heads_v, x_v, tok_v, gm_v, gf_v,
                w_sem, h_sem, d_send, d_recv, x_send, x_recv, g_send, g_recv, f_send, f_recv, s_send, s_recv):
    me = lax.axis_index('tp')
    n_tp = 2 * xs.shape[1]
    chips = n_tp // 2
    xi, core = me // 2, me % 2
    sibling = {'tp': me + 1 - 2 * core}
    rows, width = p_s.shape
    half = rows // 2
    piece = half // chips
    ff = wg.shape[1]
    vocab = wh.shape[0]
    full = vocab // CHUNK
    rest = vocab - full * CHUNK

    def rows_of(side, chip):
        return pl.ds(pl.multiple_of(side * half + chip * piece, piece), piece)

    mine = rows_of(core, xi)

    small = [pltpu.make_async_copy(x.at[mine], x_v, w_sem.at[0]), pltpu.make_async_copy(tok, tok_v, w_sem.at[1]),
             pltpu.make_async_copy(gm, gm_v, w_sem.at[2]), pltpu.make_async_copy(gf, gf_v, w_sem.at[3]),
             pltpu.make_async_copy(heads, heads_v, w_sem.at[15]),
             pltpu.make_async_copy(wo, buf.at[SLOTS - 1, pl.ds(0, wo.shape[0])], w_sem.at[16])]
    last_copy = pltpu.make_async_copy(wh.at[pl.ds(full * CHUNK, rest)], last_v, w_sem.at[4])
    mlp_copies = []
    for n, w in enumerate((wg, wu)):
        for kb in range(width // CHUNK):
            mlp_copies.append(pltpu.make_async_copy(
                w.at[pl.ds(kb * CHUNK, CHUNK)], buf.at[2 * n + kb // 2, :, pl.ds((kb % 2) * ff, ff)],
                w_sem.at[5 + 4 * n + kb]))
    for kb in range(ff // CHUNK):
        mlp_copies.append(pltpu.make_async_copy(wd.at[pl.ds(kb * CHUNK, CHUNK)], buf.at[4 + kb], w_sem.at[13 + kb]))

    def slot_of(i):
        return lax.rem(i + MLP_SLOTS, SLOTS)

    def head_copy(i):
        return pltpu.make_async_copy(wh.at[pl.ds(pl.multiple_of(i * CHUNK, CHUNK), CHUNK)], buf.at[slot_of(i)],
                                     h_sem.at[slot_of(i)])

    def head_begin(i, carry):
        head_copy(i).start()
        return carry

    for copy in small:
        copy.start()
    lax.fori_loop(0, EARLY, head_begin, 0)
    for copy in mlp_copies:
        copy.start()
    lax.fori_loop(EARLY, SLOTS - MLP_SLOTS - 1, head_begin, 0)
    last_copy.start()

    barrier = pltpu.get_barrier_semaphore()
    for k in range(1, n_tp):
        pl.semaphore_signal(barrier, inc=1, device_id={'tp': lax.rem(me + k, n_tp)}, device_id_type=MESH)

    acd[0] = jnp.full((8, rows), LOW, F32)
    acd[1] = jnp.zeros((8, rows), F32)
    acd[2] = jnp.zeros((8, rows), F32)
    acc[0] = jnp.full((rows, 128), LOW, F32)
    acc[1] = jnp.zeros((rows, 128), F32)
    acc[2] = jnp.zeros((rows, 128), F32)
    for copy in small:
        copy.wait()
    tok_row = (tok_v[...].reshape(1, rows) - me * vocab).astype(F32)
    tok_row = jnp.where((tok_row >= 0) & (tok_row < vocab), tok_row, -float(2 * vocab))
    tok_r[...] = jnp.broadcast_to(tok_row, (8, rows)).astype(jnp.int32)
    tok_c[...] = jnp.transpose(jnp.broadcast_to(tok_row, (rows, rows))).astype(jnp.int32)

    o_s[...] = jnp.dot(heads_v[...], buf[SLOTS - 1, :wo.shape[0], :], preferred_element_type=F32).astype(BF16)
    head_copy(SLOTS - MLP_SLOTS - 1).start()
    pl.semaphore_wait(barrier, n_tp - 1)

    turned = [0]

    def chew(count):
        first = turned[0]
        turned[0] += count

        def one(i, carry):
            head_copy(i).wait()
            slot = slot_of(i)

            def strip(c, inner):
                cols = pl.ds(pl.multiple_of(c * CHUNK, CHUNK), CHUNK)
                buf[slot, :, cols] = jnp.transpose(buf[slot, :, cols])
                return inner

            lax.fori_loop(0, width // CHUNK, strip, 0)
            return carry

        if count:
            lax.fori_loop(first, first + count, one, 0)

    def exchange(rnd, src, full_ref, finish, landed):
        order = [2, 1, 3]

        def pair_copy(k):
            chip = lax.rem(xi + k, chips)
            return pltpu.make_async_remote_copy(
                src_ref=src.at[rows_of(1 - core, chip)], dst_ref=d2d.at[rnd, k],
                send_sem=d_send.at[rnd, k], recv_sem=d_recv.at[rnd, k], device_id=sibling, device_id_type=MESH)

        def ring_copy(k):
            return pltpu.make_async_remote_copy(
                src_ref=xs.at[rnd, k], dst_ref=xr.at[rnd, k], send_sem=x_send.at[rnd, k], recv_sem=x_recv.at[rnd, k],
                device_id={'tp': lax.rem(xi + k, chips) * 2 + core}, device_id_type=MESH)

        def share_copy(k):
            return pltpu.make_async_remote_copy(
                src_ref=full_ref.at[mine], dst_ref=full_ref.at[mine], send_sem=g_send.at[rnd, k], recv_sem=g_recv.at[rnd, k],
                device_id={'tp': lax.rem(xi + k, chips) * 2 + core}, device_id_type=MESH)

        def forward_copy(k):
            its = rows_of(core, lax.rem(xi + chips - k, chips))
            return pltpu.make_async_remote_copy(
                src_ref=full_ref.at[its], dst_ref=full_ref.at[its], send_sem=f_send.at[rnd, k], recv_sem=f_recv.at[rnd, k],
                device_id=sibling, device_id_type=MESH)

        for k in order + [0]:
            pair_copy(k).start()
        chew(CHEW[rnd][0])
        for k in order:
            pair_copy(k).wait_recv()
            chip = lax.rem(xi + k, chips)
            xs[rnd, k] = (src[rows_of(core, chip), :].astype(F32) + d2d[rnd, k].astype(F32)).astype(BF16)
            ring_copy(k).start()
        pair_copy(0).wait_recv()
        chew(CHEW[rnd][1])
        total = src[mine, :].astype(F32) + d2d[rnd, 0].astype(F32)
        for k in (1, 3, 2):
            ring_copy(k).wait_recv()
            total = total + xr[rnd, k].astype(F32)
        full_ref[mine, :] = finish(total)
        for k in order:
            share_copy(k).start()
        forward_copy(0).start()
        chew(CHEW[rnd][2])
        for k in (1, 3, 2):
            share_copy(k).wait_recv()
            forward_copy(k).start()
        landed(core)
        for k in range(chips):
            forward_copy(k).wait_recv()
        landed(1 - core)
        for k in range(chips):
            pair_copy(k).wait_send()
            forward_copy(k).wait_send()
            if k:
                ring_copy(k).wait_send()
                share_copy(k).wait_send()

    def finish_attn(total):
        a = (x_v[...].astype(F32) + total).astype(BF16)
        a_s[...] = a
        return rms(a.astype(F32), gm_v[...].astype(F32).reshape(1, -1))

    exchange(0, o_s, m_s, finish_attn, lambda side: None)

    for copy in mlp_copies:
        copy.wait()

    def widen(n):
        out = None
        for kb in range(width // CHUNK):
            term = jnp.dot(m_s[:, kb * CHUNK:(kb + 1) * CHUNK], buf[2 * n + kb // 2, :, (kb % 2) * ff:(kb % 2 + 1) * ff],
                           preferred_element_type=F32)
            out = term if out is None else out + term
        return out

    gate = widen(0)
    h_s[...] = (gate * jax.nn.sigmoid(gate) * widen(1)).astype(BF16)
    p_s[...] = (jnp.dot(h_s[:, :CHUNK], buf[4], preferred_element_type=F32)
                + jnp.dot(h_s[:, CHUNK:], buf[5], preferred_element_type=F32)).astype(BF16)
    lax.fori_loop(SLOTS - MLP_SLOTS, SLOTS, head_begin, 0)

    def final_norm(side):
        band = pl.ds(pl.multiple_of(side * half, half), half)
        f_s[band, :] = rms(y_s[band, :].astype(F32), gf_v[...].astype(F32).reshape(1, -1))

    exchange(1, p_s, y_s, lambda total: (a_s[...].astype(F32) + total).astype(BF16), final_norm)
    y_copy = pltpu.make_async_copy(y_s, y_out, w_sem.at[17])
    y_copy.start()

    lane = lax.broadcasted_iota(jnp.int32, (rows, 128), 1)

    def fold_across(scores, first_row):
        parts = [scores[:, j * 128:(j + 1) * 128] for j in range(scores.shape[1] // 128)]
        old = acc[0]
        top = functools.reduce(jnp.maximum, parts, old)
        total = acc[1] * jnp.exp(old - top)
        target = acc[2]
        place = tok_c[...] - first_row
        for j, part in enumerate(parts):
            total = total + jnp.exp(part - top)
            target = target + jnp.where(place == lane + j * 128, part, 0.0)
        acc[0] = top
        acc[1] = total
        acc[2] = target

    def fold_down(scores, first_row):
        groups = scores.reshape(scores.shape[0] // 8, 8, rows)
        old = acd[0]
        top = jnp.maximum(old, jnp.max(groups, axis=0))
        acd[1] = acd[1] * jnp.exp(old - top) + jnp.sum(jnp.exp(groups - top[None]), axis=0)
        ids = lax.broadcasted_iota(jnp.int32, scores.shape, 0)
        hit = ids == (tok_r[0:1, :] - first_row)
        acd[2] = acd[2] + jnp.sum(jnp.where(hit, scores, 0.0).reshape(groups.shape), axis=0)
        acd[0] = top

    def turned_chunk(i):
        slot = slot_of(i)
        scores = []
        for r in range(CHUNK // BLOCK):
            out = None
            for c in range(width // CHUNK):
                for n in range(CHUNK // BLOCK):
                    term = jnp.dot(f_s[:, c * CHUNK + n * BLOCK:c * CHUNK + (n + 1) * BLOCK],
                                   buf[slot, n * BLOCK:(n + 1) * BLOCK, c * CHUNK + r * BLOCK:c * CHUNK + (r + 1) * BLOCK],
                                   preferred_element_type=F32)
                    out = term if out is None else out + term
            scores.append(out)
        fold_across(jnp.concatenate(scores, axis=1), i * CHUNK)

    def plain_chunk(i):
        scores = lax.dot_general(buf[slot_of(i)], f_s[...], NT, preferred_element_type=F32)
        fold_down(scores, i * CHUNK)

    def refill(i):
        @pl.when(i + SLOTS < full)
        def _():
            head_copy(i + SLOTS).start()

    def sweep(first, count, size, take, fresh):
        def run(n, carry):
            at = [first + n * size + u for u in range(size)]
            if fresh:
                for i in at:
                    head_copy(i).wait()
            for i in at:
                take(i)
            for i in at:
                refill(i)
            return carry

        if count >= size:
            lax.fori_loop(0, count // size, run, 0)
        if count % size:
            sweep(first + count // size * size, count % size, count % size, take, fresh)

    sweep(0, turned[0], GROUP, turned_chunk, False)
    sweep(turned[0], full - turned[0], GROUP, plain_chunk, True)
    last_copy.wait()
    fold_down(lax.dot_general(last_v[...], f_s[...], NT, preferred_element_type=F32), full * CHUNK)

    tops = jnp.transpose(acc[0])
    top = jnp.maximum(jnp.max(tops, axis=0, keepdims=True), jnp.max(acd[0], axis=0, keepdims=True))
    total = (jnp.sum(jnp.transpose(acc[1]) * jnp.exp(tops - top), axis=0, keepdims=True)
             + jnp.sum(acd[1] * jnp.exp(acd[0] - top), axis=0, keepdims=True))
    target = jnp.sum(jnp.transpose(acc[2]), axis=0, keepdims=True) + jnp.sum(acd[2], axis=0, keepdims=True)
    st_s[...] = jnp.concatenate([top, total, target, jnp.zeros((5, rows), F32)], axis=0)

    def stat_copy(k):
        return pltpu.make_async_remote_copy(
            src_ref=st_s, dst_ref=st_r.at[k], send_sem=s_send.at[k], recv_sem=s_recv.at[k],
            device_id={'tp': lax.rem(me + k, n_tp)}, device_id_type=MESH)

    for k in range(1, n_tp):
        stat_copy(k).start()
    y_copy.wait()
    for k in range(1, n_tp):
        stat_copy(k).wait_recv()
    tops = [top] + [st_r[k, 0:1, :] for k in range(1, n_tp)]
    totals = [total] + [st_r[k, 1:2, :] for k in range(1, n_tp)]
    best = functools.reduce(jnp.maximum, tops)
    mass = sum(s * jnp.exp(t - best) for s, t in zip(totals, tops))
    hit = target + sum(st_r[k, 2:3, :] for k in range(1, n_tp))
    lse = best + jnp.log(mass)
    stats[...] = jnp.concatenate([hit - lse, lse, jnp.zeros((6, rows), F32)], axis=0)
    for k in range(1, n_tp):
        stat_copy(k).wait_send()


def tail(heads, x, tok, gm, gf, wo, wg, wu, wd, wh, n_tp):
    rows, width = x.shape
    chips = n_tp // 2
    piece = rows // n_tp
    vmem = pl.BlockSpec(memory_space=pltpu.VMEM)
    hbm = pl.BlockSpec(memory_space=pltpu.HBM)
    dma = pltpu.SemaphoreType.DMA
    rest = wh.shape[0] % CHUNK
    return pl.pallas_call(
        tail_kernel,
        out_shape=(jax.ShapeDtypeStruct((rows, width), BF16), jax.ShapeDtypeStruct((8, rows), F32)),
        in_specs=[hbm] * 10,
        out_specs=(hbm, vmem),
        scratch_shapes=[pltpu.VMEM((SLOTS, CHUNK, width), BF16), pltpu.VMEM((rows, width), BF16), pltpu.VMEM((rest, width), BF16),
                        pltpu.VMEM((2, chips, piece, width), BF16), pltpu.VMEM((2, chips, piece, width), BF16),
                        pltpu.VMEM((2, chips, piece, width), BF16),
                        pltpu.VMEM((rows, width), BF16), pltpu.VMEM((piece, width), BF16),
                        pltpu.VMEM((rows, wg.shape[1]), BF16),
                        pltpu.VMEM((rows, width), BF16), pltpu.VMEM((rows, width), BF16),
                        pltpu.VMEM((rows, width), BF16), pltpu.VMEM((3, rows, 128), F32), pltpu.VMEM((3, 8, rows), F32),
                        pltpu.VMEM((rows, rows), jnp.int32), pltpu.VMEM((8, rows), jnp.int32),
                        pltpu.VMEM((8, rows), F32), pltpu.VMEM((n_tp, 8, rows), F32),
                        pltpu.VMEM(heads.shape, BF16), pltpu.VMEM((piece, width), BF16), pltpu.VMEM((rows,), jnp.int32),
                        pltpu.VMEM(gm.shape, BF16), pltpu.VMEM(gf.shape, BF16),
                        dma((18,)), dma((SLOTS,)),
                        dma((2, chips)), dma((2, chips)), dma((2, chips)), dma((2, chips)),
                        dma((2, chips)), dma((2, chips)), dma((2, chips)), dma((2, chips)),
                        dma((n_tp,)), dma((n_tp,))],
        compiler_params=pltpu.CompilerParams(vmem_limit_bytes=VMEM_TAIL, collective_id=0, has_side_effects=True),
        name='tail',
    )(heads, x, tok, gm, gf, wo, wg, wu, wd, wh)


VMEM_TAIL = VMEM_ALL


PIECES = 4


def give_kernel(y, stats, y_out, logp_out, lse_out, y_v, s_v, logp_v, lse_v, in_sem, out_sem, s_sem):
    band = [pl.ds(n * (y.shape[0] // PIECES), y.shape[0] // PIECES) for n in range(PIECES)]
    reads = [pltpu.make_async_copy(y.at[b], y_v.at[b], in_sem.at[n]) for n, b in enumerate(band)]
    writes = [pltpu.make_async_copy(y_v.at[b], y_out.at[b], out_sem.at[n]) for n, b in enumerate(band)]
    stat_read = pltpu.make_async_copy(stats, s_v, s_sem.at[0])
    sent = [pltpu.make_async_copy(logp_v, logp_out, s_sem.at[1]), pltpu.make_async_copy(lse_v, lse_out, s_sem.at[2])]
    stat_read.start()
    for read in reads:
        read.start()
    stat_read.wait()
    logp_v[...] = s_v[0:1, :].reshape(s_v.shape[1])
    lse_v[...] = s_v[1:2, :].reshape(s_v.shape[1])
    for copy in sent:
        copy.start()
    for read, write in zip(reads, writes):
        read.wait()
        write.start()
    for copy in writes + sent:
        copy.wait()


def give(y, stats):
    rows = y.shape[0]
    hbm = pl.BlockSpec(memory_space=pltpu.HBM)
    dma = pltpu.SemaphoreType.DMA
    return pl.pallas_call(
        give_kernel,
        out_shape=(jax.ShapeDtypeStruct(y.shape, BF16), jax.ShapeDtypeStruct((rows,), F32), jax.ShapeDtypeStruct((rows,), F32)),
        in_specs=[hbm, hbm],
        out_specs=(hbm, hbm, hbm),
        scratch_shapes=[pltpu.VMEM(y.shape, BF16), pltpu.VMEM(stats.shape, F32), pltpu.VMEM((rows,), F32), pltpu.VMEM((rows,), F32),
                        dma((PIECES,)), dma((PIECES,)), dma((3,))],
        compiler_params=pltpu.CompilerParams(vmem_limit_bytes=VMEM_ALL),
        name='give',
    )(y, stats)


def solution(mesh):
    n_tp = mesh.shape['tp']

    def local_step(tok_hidden, seq_lens, k_cache, v_cache, next_tok, g_attn, w_q, b_q, w_k, b_k, w_v, b_v, w_o, g_mlp,
                   w_gate, w_up, w_down, g_final, w_head):
        heads, k_all, v_all = attention(tok_hidden, seq_lens, k_cache, v_cache, g_attn, w_q, b_q, w_k, b_k, w_v, b_v)
        y_all, stats = tail(heads, tok_hidden, next_tok, g_mlp, g_final, w_o, w_gate, w_up, w_down, w_head, n_tp)
        y_out, tok_logp, norm_lse = give(y_all, stats)
        return y_out, k_all, v_all, tok_logp, norm_lse

    row_spec = P('dp', None)
    vec_spec = P('dp')
    cache_spec = P('dp', None, 'tp', None)
    col_spec = P(None, 'tp')
    part_spec = P('tp')
    whole_spec = P(None)
    in_specs = (row_spec, vec_spec, cache_spec, cache_spec, vec_spec, whole_spec, col_spec, part_spec, col_spec, part_spec,
                col_spec, part_spec, P('tp', None), whole_spec, col_spec, col_spec, P('tp', None), whole_spec, P('tp', None))
    out_specs = (row_spec, cache_spec, cache_spec, vec_spec, vec_spec)
    return jax.shard_map(local_step, mesh=mesh, in_specs=in_specs, out_specs=out_specs, check_vma=False)
```
